32 devices in a mesh: task: 2 (over x), batch: 16 (over z, y, core).
Axes of the slice: x: 2, y: 2, z: 4, core: 2. Of those that a mesh axis runs over, the one named last changes fastest.
Arguments:
- pooled: bfloat16 [12288, 3328], P('batch'), may hold values from -6 to 6
- gate_weight: bfloat16 [3328, 8, 4], P(None, 'task'), may hold values from -0.21875 to 0.21875
- w_first: bfloat16 [8, 3328, 1024], P('task', 'batch'), may hold values from -0.15625 to 0.15625
- w_second: bfloat16 [8, 1024, 512], P('task', 'batch'), may hold values from -0.25 to 0.25
- w_third: bfloat16 [8, 512, 256], P('task', 'batch'), may hold values from -0.375 to 0.375
- tower_hidden: bfloat16 [4, 256, 128], P('task'), may hold values from -0.5 to 0.5
- tower_out: bfloat16 [4, 128], P('task'), may hold values from -0.75 to 0.75
Outputs:
- task_logits: float32 [12288, 4], P('batch', 'task')
The draws below stay inside these ranges and needn't reach their ends.
All inputs are finite; a program needn't handle non-finite values.
Results may differ from the reference program's by a relative error of at most 0.02.
Values may be sent and summed in bfloat16 or wider, within the bound.
A program may use at most 128 MiB of HBM per device.

```python
import jax
import jax.numpy as jnp

H1 = 1024
H2 = 512
H3 = 256
TOWER = 128
TASKS = 4
D_IN = 3328
EXPERTS = 8
TOKENS = 12288


def steps_of(own_key, extent, shards, smallest, largest):
    def one(position, parts):
        heights = jax.random.uniform(jax.random.fold_in(jax.random.fold_in(own_key, 6), position), (parts,), jnp.float32, smallest / len(shards), largest / len(shards))
        return jnp.repeat(jnp.exp(heights), extent[position] // parts).reshape((-1,) + (1,) * (len(extent) - position - 1))

    loudness = one(*shards[0])
    for cut in shards[1:]:
        loudness = loudness * one(*cut)
    return loudness


def centred(key, extent, width, limit, shards=(), kind=jnp.bfloat16):
    gain = steps_of(key, extent, shards, -0.22, 0.18) if shards else 1.0
    values = jax.random.normal(key, extent, jnp.float32) * width * gain
    return jnp.minimum(jnp.maximum(values, -limit), limit).astype(kind)


def setup_inputs(seed: int = 0) -> dict:
    streams_of = jax.random.split(jax.random.key(seed), 8)
    return {
        "pooled": centred(streams_of[0], (TOKENS, D_IN), 1.0, 6.0, ((0, 16),)),
        "gate_weight": centred(streams_of[1], (D_IN, EXPERTS, TASKS), (D_IN // 4) ** -0.5, 0.21875, ((1, 2),)),
        "w_first": centred(streams_of[2], (EXPERTS, D_IN, H1), (D_IN // 2) ** -0.5, 0.15625, ((0, 2), (1, 16))),
        "w_second": centred(streams_of[3], (EXPERTS, H1, H2), (H1 // 2) ** -0.5, 0.25, ((0, 2), (1, 16))),
        "w_third": centred(streams_of[4], (EXPERTS, H2, H3), (H2 // 2) ** -0.5, 0.375, ((0, 2), (1, 16))),
        "tower_hidden": centred(streams_of[5], (TASKS, H3, TOWER), (H3 // 2) ** -0.5, 0.5, ((0, 2),)),
        "tower_out": centred(streams_of[6], (TASKS, TOWER), (TOWER // 2) ** -0.5, 0.75, ((0, 2),)),
    }


def reference(pooled, gate_weight, w_first, w_second, w_third, tower_hidden, tower_out):
    logits = jnp.dot(pooled, gate_weight.reshape(D_IN, EXPERTS * TASKS), preferred_element_type=jnp.float32)
    logits = logits.reshape(TOKENS, EXPERTS, TASKS)
    weights = jnp.exp(logits)
    total = jnp.sum(weights, axis=1)
    numer = jnp.zeros((TOKENS, TASKS, H3), jnp.float32)
    for expert_id in range(EXPERTS):
        first = jax.nn.relu(jnp.dot(pooled, w_first[expert_id], preferred_element_type=jnp.float32)).astype(jnp.bfloat16)
        second = jax.nn.relu(jnp.dot(first, w_second[expert_id], preferred_element_type=jnp.float32)).astype(jnp.bfloat16)
        expert_out = jax.nn.relu(jnp.dot(second, w_third[expert_id], preferred_element_type=jnp.float32)).astype(jnp.bfloat16)
        numer = numer + weights[:, expert_id, :][:, :, None] * expert_out.astype(jnp.float32)[:, None, :]
    mix = (numer / total[:, :, None]).astype(jnp.bfloat16)
    tower = jax.nn.relu(jnp.einsum("sth,thk->stk", mix.astype(jnp.float32), tower_hidden.astype(jnp.float32))).astype(jnp.bfloat16)
    return jnp.einsum("stk,tk->st", tower.astype(jnp.float32), tower_out.astype(jnp.float32))
```

```python
import functools

import jax
import jax.numpy as jnp
from jax import lax
from jax.experimental import pallas as pl
from jax.experimental.pallas import tpu as pltpu
from jax.sharding import PartitionSpec as P

MESH = pl.DeviceIdType.MESH
BF16, F32 = jnp.bfloat16, jnp.float32
VMEM_BYTES = 63 * 1024 * 1024
BLOCKS, PIECES = 4, 8


def dot(a, b):
    return jnp.dot(a, b, preferred_element_type=F32)


def fused_kernel(
    nb, pieces,
    pooled, gate, w_first, w_second, w_third, tower_hidden, tower_out, out,
    tok, buf, dbuf, first, out_tx, out_rx, gate_rx, gate_all, wts, acc, th_all, to_all, res, res_rx,
    loc, loc_deep, loc_tok, y_s, y_r, yd_s, yd_r, p_s, p_r, q_s, q_r, g_s, g_r,
    z_r, up_s, dn_s, sib_r, sib_s, o_s, o_r, r_s, r_r,
):
    t, b = lax.axis_index("task"), lax.axis_index("batch")
    nz = nb // 4
    z, y, c = b // 4, (b // 2) % 2, b % 2
    chunks, wide = buf.shape[0], buf.shape[5]
    group = dbuf.shape[3]
    blocks = chunks // group
    tokens = pooled.shape[0]
    half = tokens // 2
    piece = half // pieces
    tasks = tower_hidden.shape[0]
    experts = gate.shape[0]
    deep_rows = w_second.shape[1]
    width = w_third.shape[2]
    splits = w_second.shape[2] // width
    deep = chunks

    def at(zz, yy, cc):
        return zz * 4 + yy * 2 + cc

    across, sib = at(z, 1 - y, c), at(z, y, 1 - c)
    up, down = at(z + 1, y, c), at(z - 1, y, c)

    def remote(src, dst, send, recv, tt, bb):
        return pltpu.make_async_remote_copy(
            src_ref=src, dst_ref=dst, send_sem=send, recv_sem=recv,
            device_id=(tt, bb), device_id_type=MESH,
        )

    def shard(k, yy):
        cols = pl.ds(pl.multiple_of((k % blocks) * wide, 128), wide)
        return w_first.at[yy * group + k // blocks, :, cols]

    def own_copy(k):
        return pltpu.make_async_copy(shard(k, y), buf.at[k, z, y, c], loc.at[k])

    def deep_parts(yy):
        own = pl.ds(yy * group, group)
        to = dbuf.at[z, y, c]
        parts = [
            (w_second.at[own, :, pl.ds(h * width, width)],
             to.at[:, pl.ds(h * deep_rows, deep_rows)])
            for h in range(splits)
        ]
        return parts + [(w_third.at[own], to.at[:, pl.ds(splits * deep_rows, w_third.shape[1])])]

    deep_copies = [
        pltpu.make_async_copy(src, dst, loc_deep.at[n])
        for n, (src, dst) in enumerate(deep_parts(y))
    ]
    deep_across = [
        remote(src, dst, yd_s.at[n], yd_r.at[n], t, across)
        for n, (src, dst) in enumerate(deep_parts(1 - y))
    ]
    tok_copy = pltpu.make_async_copy(pooled, tok.at[pl.ds(0, tokens)], loc_tok.at[0])

    for copy in deep_copies:
        copy.start()

    @pl.loop(0, chunks)
    def _(k):
        own_copy(k).start()

    tok_copy.start()

    barrier = pltpu.get_barrier_semaphore()
    for tt, bb in (
        (t, across), (t, sib), (t, at((z + 1) % nz, y, c)), (t, at((z + nz - 1) % nz, y, c)),
        (1 - t, b), (1 - t, across),
    ):
        pl.semaphore_signal(barrier, inc=1, device_id=(tt, bb), device_id_type=MESH)
    pl.semaphore_wait(barrier, 6)

    def y_move(k):
        return remote(shard(k, 1 - y), buf.at[k, z, y, c], y_s.at[k], y_r.at[k], t, across)

    def tok_rows(h, p):
        return pl.ds(pl.multiple_of(h * half + p * piece, 16), piece)

    def p_move(p):
        rows = pl.ds(pl.multiple_of(tokens + t * half + p * piece, 16), piece)
        return remote(pooled.at[tok_rows(t, p)], tok.at[rows], p_s.at[p], p_r.at[p], t, across)

    def q_move(p):
        rows = pl.ds(pl.multiple_of(tokens + t * half + p * piece, 16), piece)
        return remote(tok.at[rows], tok.at[rows], q_s.at[p], q_r.at[p], 1 - t, b)

    swaps = [
        remote(gate, gate_rx, g_s.at[0], g_r.at[0], 1 - t, b),
        remote(tower_hidden, th_all.at[pl.ds(t * tasks, tasks)], g_s.at[1], g_r.at[1], 1 - t, b),
        remote(tower_out, to_all.at[t], g_s.at[2], g_r.at[2], 1 - t, b),
    ]

    for move in deep_across:
        move.start()
    y_move(0).start()
    y_move(1).start()
    p = 0
    for k in range(2, chunks):
        for _ in range(4 if k == 2 else 2):
            if p < pieces:
                p_move(p).start()
                p += 1
        y_move(k).start()
    for move in swaps:
        move.start()

    def pair(k, zz):
        if k is deep:
            return dbuf.at[zz, :, c]
        return buf.at[k, zz, :, c]

    def slot(k, yy):
        if k is deep:
            return dbuf.at[z, yy, c]
        return buf.at[k, z, yy, c]

    def row(k):
        return chunks if k is deep else k

    def z_own(k, yy, n, what):
        ref = slot(k, yy)

        @pl.when(z < nz - 1)
        def _():
            what(remote(ref, ref, up_s.at[row(k), n], z_r.at[row(k), z], t, up))

        @pl.when(z > 0)
        def _():
            what(remote(ref, ref, dn_s.at[row(k), n], z_r.at[row(k), z], t, down))

    def z_up(k, zz):
        return remote(pair(k, zz), pair(k, zz), up_s.at[row(k), zz], z_r.at[row(k), zz], t, up)

    def z_down(k, zz):
        return remote(pair(k, zz), pair(k, zz), dn_s.at[row(k), zz], z_r.at[row(k), zz], t, down)

    def sib_move(k, zz):
        return remote(pair(k, zz), pair(k, zz), sib_s.at[row(k), zz], sib_r.at[row(k), zz], t, sib)

    def start(copy):
        copy.start()

    def own_start(k):
        if k is deep:
            for copy in deep_copies:
                copy.wait()
        else:
            own_copy(k).wait()
        z_own(k, y, z, start)

    def own_finish(k):
        if k is deep:
            for move in deep_across:
                move.wait_recv()
        else:
            y_move(k).wait_recv()
        z_own(k, 1 - y, nz, start)
        sib_move(k, z).start()

    def z_step(k, d):
        @pl.when(z >= d)
        def _():
            z_up(k, z - d).wait_recv()

            @pl.when(z < nz - 1)
            def _():
                z_up(k, z - d).start()

            sib_move(k, z - d).start()

        @pl.when(z + d < nz)
        def _():
            z_down(k, z + d).wait_recv()

            @pl.when(z > 0)
            def _():
                z_down(k, z + d).start()

            sib_move(k, z + d).start()

    def sib_wait(k):
        @pl.loop(0, nz)
        def _(zz):
            sib_move(k, zz).wait_recv()

    own_start(deep)
    own_start(0)
    own_finish(deep)
    own_finish(0)
    own_start(1)
    own_finish(1)
    for d in range(1, nz):
        z_step(deep, d)

    tok_copy.wait()
    for swap in swaps:
        swap.wait_recv()
    th_all[pl.ds(t * tasks, tasks)] = tower_hidden[...]
    to_all[t] = tower_out[...]
    for e in range(experts):
        n = gate.shape[1]
        gate_all[e * n : (e + 1) * n, :] = gate[e].astype(F32)
        gate_all[(experts + e) * n : (experts + e + 1) * n, :] = gate_rx[e].astype(F32)
    mine = pl.ds(pl.multiple_of(t * half, 16), half)
    wts[...] = jnp.exp(
        lax.dot_general(
            tok[mine, :], gate_all[...].astype(BF16), (((1,), (1,)), ((), ())),
            preferred_element_type=F32,
        )
    )
    acc[...] = jnp.zeros_like(acc)
    sib_wait(deep)

    def route(g):
        near = g // 2
        owner = t + (1 - g % 2) * (1 - 2 * t)
        bb = at(z, jnp.where(near == 1, y, 1 - y), c)
        return near, owner, bb

    def from_slot(owner, i):
        return (jnp.where(owner == t, 0, 1) * 2 + y) * group + i

    def o_move(i, g):
        near, owner, bb = route(g)
        n = from_slot(owner, i)
        return remote(out_tx.at[i, g], out_rx.at[n], o_s.at[i, g], o_r.at[n], owner, bb)

    def compute(k, g):
        near, owner, _ = route(g)
        rows = pl.ds(pl.multiple_of((1 - near) * tokens + owner * half, 16), half)
        cols = pl.ds(pl.multiple_of((k % blocks) * wide, 128), wide)
        weights = buf[k].reshape(-1, wide)
        first[rows, cols] = jnp.maximum(dot(tok[rows, :], weights), 0.0).astype(BF16)

        @pl.when(k % blocks == blocks - 1)
        def _():
            i = k // blocks
            hidden = first[rows, :]
            w3 = dbuf[:, :, :, i, pl.ds(splits * deep_rows, w_third.shape[1]), :].reshape(-1, width)
            total = None
            for h in range(splits):
                w2 = dbuf[:, :, :, i, pl.ds(h * deep_rows, deep_rows), :].reshape(-1, width)
                second = jnp.maximum(dot(hidden, w2), 0.0).astype(BF16)
                part = dot(second, w3[h * width : (h + 1) * width])
                total = part if total is None else total + part
            value = jnp.maximum(total, 0.0).astype(BF16)

            @pl.when(g < 3)
            def _():
                out_tx[i, g] = value
                o_move(i, g).start()

            @pl.when(g == 3)
            def _():
                out_rx[from_slot(t, i)] = value

    def accumulate(far, yy, i):
        value = out_rx[(far * 2 + yy) * group + i].astype(F32)
        n = gate.shape[1]
        for j in range(n):
            col = (far * experts + yy * group + i) * n + j
            acc[j] = acc[j] + wts[:, col : col + 1] * value

    def mix_in(i):
        for far in range(2):
            for yy in range(2):
                n = (far * 2 + yy) * group + i

                def waiting():
                    remote(out_tx.at[i, 0], out_rx.at[n], o_s.at[i, 0], o_r.at[n], t, across).wait_recv()

                if far == 0:
                    pl.when(y != yy)(waiting)
                else:
                    waiting()
                accumulate(far, yy, i)

    def lag(j):
        most = jnp.minimum(j + 1, jnp.maximum(0, 2 * (j - 2)))
        return jnp.where(j == chunks - 1, chunks, most)

    first_lag = 3
    per = -(-pieces // first_lag)

    @pl.loop(0, chunks)
    def _(i):
        @pl.when(i + 2 < chunks)
        def _():
            own_start(i + 2)
            own_finish(i + 2)

        @pl.when(i >= 1)
        def _():
            sib_wait(i - 1)
            compute(i - 1, 2)

        z_step(i, 1)

        @pl.when(i >= 1)
        def _():
            compute(i - 1, 3)

        for d in range(2, nz - 1):
            z_step(i, d)

        @pl.when(i == first_lag + 1)
        def _():
            @pl.loop(0, pieces)
            def _(p):
                q_move(p).wait_recv()

        @pl.when(i > first_lag)
        def _():
            @pl.loop(lag(i - 2), lag(i - 1))
            def _(k):
                compute(k, 0)
                compute(k, 1)

        z_step(i, nz - 1)

        @pl.when(jnp.logical_and(i >= 1, i <= first_lag))
        def _():
            @pl.loop((i - 1) * per, jnp.minimum(i * per, pieces))
            def _(p):
                p_move(p).wait_recv()
                q_move(p).start()

        @pl.when(i == chunks - 1)
        def _():
            for i in range(group - 1):
                mix_in(i)

    last = chunks - 1
    sib_wait(last)

    @pl.loop(lag(last - 1), last)
    def _(k):
        compute(k, 0)
        compute(k, 1)

    @pl.loop(0, 4)
    def _(g):
        compute(last, g)

    mix_in(group - 1)

    n = gate.shape[1]
    for j in range(n):
        total = None
        for e in range(2 * experts):
            w = wts[:, e * n + j : e * n + j + 1]
            total = w if total is None else total + w
        mix = (acc[j] / total).astype(BF16)
        tower = jnp.maximum(dot(mix, th_all[j]), 0.0).astype(BF16)
        vector = jnp.broadcast_to(to_all[j // tasks, j % tasks : j % tasks + 1, :], (16, tower.shape[1]))
        line = lax.dot_general(
            vector, tower, (((1,), (1,)), ((), ())), preferred_element_type=F32
        )
        res[j // tasks, j % tasks : j % tasks + 1, :] = line[:1]
    r_move = remote(res.at[1 - t], res_rx, r_s.at[0], r_r.at[0], 1 - t, b)
    r_move.start()
    out[:, pl.ds(pl.multiple_of(t * half, 128), half)] = res[t, 0:tasks, :]

    for move in deep_across:
        move.wait_send()
    for swap in swaps:
        swap.wait_send()

    @pl.loop(0, pieces)
    def _(p):
        p_move(p).wait_send()
        q_move(p).wait_send()

    for i in range(group):
        @pl.loop(0, 3)
        def _(g):
            o_move(i, g).wait_send()

    def sent(k):
        z_own(k, y, z, lambda copy: copy.wait_send())
        z_own(k, 1 - y, nz, lambda copy: copy.wait_send())

        @pl.loop(0, nz)
        def _(zz):
            sib_move(k, zz).wait_send()

            @pl.when(jnp.logical_and(z < nz - 1, zz < z))
            def _():
                z_up(k, zz).wait_send()

            @pl.when(jnp.logical_and(z > 0, zz > z))
            def _():
                z_down(k, zz).wait_send()

    sent(deep)

    @pl.loop(0, chunks)
    def _(k):
        y_move(k).wait_send()
        sent(k)

    r_move.wait()
    out[:, pl.ds(pl.multiple_of((1 - t) * half, 128), half)] = res_rx[0:tasks, :]


def fused(nb, pooled, gate_weight, w_first, w_second, w_third, tower_hidden, tower_out):
    tokens, width_in = pooled.shape
    experts, rows, h1 = w_first.shape
    tasks = tower_hidden.shape[0]
    all_tasks = gate_weight.shape[2]
    deep_rows, deep_width = w_second.shape[1:]
    last_rows, last_width = w_third.shape[1:]
    nz = nb // 4
    group = experts // 2
    wide = h1 // BLOCKS
    chunks = group * BLOCKS
    half = tokens // 2
    splits = deep_width // last_width
    packed_rows = splits * deep_rows + last_rows
    dma = pltpu.SemaphoreType.DMA
    vmem = pl.BlockSpec(memory_space=pltpu.VMEM)
    anywhere = pl.BlockSpec(memory_space=pl.ANY)
    gate = jnp.transpose(gate_weight, (1, 2, 0))
    lines = pl.pallas_call(
        functools.partial(fused_kernel, nb, PIECES),
        out_shape=jax.ShapeDtypeStruct((tasks, tokens), F32),
        in_specs=[anywhere, vmem, anywhere, anywhere, anywhere, vmem, vmem],
        out_specs=vmem,
        scratch_shapes=[
            pltpu.VMEM((2 * tokens, width_in), BF16),
            pltpu.VMEM((chunks, nz, 2, 2, rows, wide), BF16),
            pltpu.VMEM((nz, 2, 2, group, packed_rows, last_width), BF16),
            pltpu.VMEM((2 * tokens, h1), BF16),
            pltpu.VMEM((group, 3, half, last_width), BF16),
            pltpu.VMEM((4 * group, half, last_width), BF16),
            pltpu.VMEM(gate.shape, BF16),
            pltpu.VMEM((2 * experts * all_tasks, width_in), F32),
            pltpu.VMEM((half, 2 * experts * all_tasks), F32),
            pltpu.VMEM((all_tasks, half, last_width), F32),
            pltpu.VMEM((all_tasks,) + tower_hidden.shape[1:], BF16),
            pltpu.VMEM((2,) + tower_out.shape, BF16),
            pltpu.VMEM((2, 8, half), F32),
            pltpu.VMEM((8, half), F32),
            dma((chunks,)),
            dma((splits + 1,)),
            dma((1,)),
            dma((chunks,)),
            dma((chunks,)),
            dma((splits + 1,)),
            dma((splits + 1,)),
            dma((PIECES,)),
            dma((PIECES,)),
            dma((PIECES,)),
            dma((PIECES,)),
            dma((3,)),
            dma((3,)),
            dma((chunks + 1, nz)),
            dma((chunks + 1, nz + 1)),
            dma((chunks + 1, nz + 1)),
            dma((chunks + 1, nz)),
            dma((chunks + 1, nz)),
            dma((group, 3)),
            dma((4 * group,)),
            dma((1,)),
            dma((1,)),
        ],
        compiler_params=pltpu.CompilerParams(
            collective_id=0, has_side_effects=True, vmem_limit_bytes=VMEM_BYTES
        ),
    )(pooled, gate, w_first, w_second, w_third, tower_hidden, tower_out)
    return lines.T


def gathered_first(pooled, gate_weight, w_first, w_second, w_third, tower_hidden, tower_out):
    tok_rows = pooled.shape[0]
    width_in = pooled.shape[1]
    local_experts = w_first.shape[0]
    all_tasks = gate_weight.shape[2]
    own_tasks = tower_hidden.shape[0]
    gathered = lax.all_gather(w_first, "batch", axis=1, tiled=True)
    deep_rows, deep_width = w_second.shape[1], w_second.shape[2]
    last_rows, last_width = w_third.shape[1], w_third.shape[2]
    halves = deep_width // last_width
    packed = jnp.concatenate(
        [w_second[:, :, i * last_width : (i + 1) * last_width] for i in range(halves)] + [w_third],
        axis=1,
    )
    gathered, packed = lax.optimization_barrier((gathered, packed))
    packed = lax.all_gather(packed, "batch", axis=1, tiled=False)
    second_all = jnp.concatenate(
        [packed[:, :, i * deep_rows : (i + 1) * deep_rows] for i in range(halves)], axis=3
    ).reshape(local_experts, -1, deep_width)
    third_all = packed[:, :, halves * deep_rows :].reshape(local_experts, -1, last_width)
    summed = jnp.einsum("tr,erh->eth", pooled, gathered, preferred_element_type=jnp.float32)
    first = jax.nn.relu(summed).astype(jnp.bfloat16)
    logits = jnp.dot(
        pooled,
        gate_weight.reshape(width_in, local_experts * all_tasks),
        preferred_element_type=jnp.float32,
    )
    weights = jnp.exp(logits.reshape(tok_rows, local_experts, all_tasks))
    gate_total = jnp.sum(weights, axis=1)
    columns = first
    second = jax.nn.relu(
        jnp.einsum(
            "etr,erh->eth",
            columns,
            second_all,
            preferred_element_type=jnp.float32,
        )
    ).astype(jnp.bfloat16)
    columns = second
    expert_out = jax.nn.relu(
        jnp.einsum(
            "etr,erh->eth",
            columns,
            third_all,
            preferred_element_type=jnp.float32,
        )
    ).astype(jnp.bfloat16)
    numer = jnp.einsum("tek,eth->tkh", weights, expert_out.astype(jnp.float32))
    groups = all_tasks // own_tasks
    me = lax.axis_index("task")
    numer_own = lax.dynamic_slice_in_dim(numer, me * own_tasks, own_tasks, 1)
    total_own = lax.dynamic_slice_in_dim(gate_total, me * own_tasks, own_tasks, 1)
    for shift in range(1, groups):
        ring = [(i, (i + shift) % groups) for i in range(groups)]
        other = lax.rem(me + shift, groups) * own_tasks
        numer_sent = lax.dynamic_slice_in_dim(numer, other, own_tasks, 1).astype(jnp.bfloat16)
        total_sent = lax.dynamic_slice_in_dim(gate_total, other, own_tasks, 1)
        numer_own = numer_own + lax.ppermute(numer_sent, "task", ring).astype(jnp.float32)
        total_own = total_own + lax.ppermute(total_sent, "task", ring)
    mix = (numer_own / total_own[:, :, None]).astype(jnp.bfloat16)
    tower = jax.nn.relu(
        jnp.einsum("tkh,khm->tkm", mix, tower_hidden, preferred_element_type=jnp.float32)
    ).astype(jnp.bfloat16)
    return jnp.einsum("tkm,km->tk", tower, tower_out, preferred_element_type=jnp.float32)


def fits(mesh, pooled, gate_weight, w_first, w_second, w_third):
    even = all(w.shape[1] % 16 == 0 for w in (w_first, w_second, w_third))
    tokens, experts = pooled.shape[0], w_first.shape[0]
    cut = tokens % (32 * PIECES) == 0 and tokens % 256 == 0 and experts % 2 == 0
    lanes = w_first.shape[2] % (128 * BLOCKS) == 0 and w_second.shape[2] % w_third.shape[2] == 0
    wanted = (gate_weight.shape[1] * gate_weight.shape[2]) <= 64
    two = mesh.shape["task"] == 2 and gate_weight.shape[2] % 2 == 0
    return even and cut and lanes and wanted and two and mesh.shape["batch"] % 4 == 0


def solution(mesh):
    placed = (
        P("batch", None),
        P(None, "task", None),
        P("task", "batch", None),
        P("task", "batch", None),
        P("task", "batch", None),
        P("task", None, None),
        P("task", None),
    )

    def per_device(*args):
        if fits(mesh, *args[:5]):
            return fused(mesh.shape["batch"], *args)
        return gathered_first(*args)

    return jax.shard_map(
        per_device, mesh=mesh, in_specs=placed, out_specs=P("batch", "task"), check_vma=False
    )
```

```python
import functools

import jax
import jax.numpy as jnp
from jax import lax
from jax.experimental import pallas as pl
from jax.experimental.pallas import tpu as pltpu
from jax.sharding import PartitionSpec as P

MESH = pl.DeviceIdType.MESH
BF16, F32 = jnp.bfloat16, jnp.float32
VMEM_BYTES = 63 * 1024 * 1024
BLOCKS, PIECES = 4, 8


def dot(a, b):
    return jnp.dot(a, b, preferred_element_type=F32)


def fused_kernel(
    nb, pieces,
    pooled, gate, w_first, w_second, w_third, tower_hidden, tower_out, out,
    tok, buf, dbuf, first, out_tx, out_rx, gate_rx, gate_all, wts, acc, th_all, to_all, res, res_rx,
    loc, loc_deep, loc_tok, y_s, y_r, yd_s, yd_r, p_s, p_r, q_s, q_r, g_s, g_r,
    z_r, up_s, dn_s, sib_r, sib_s, o_s, o_r, r_s, r_r,
):
    t, b = lax.axis_index("task"), lax.axis_index("batch")
    nz = nb // 4
    z, y, c = b // 4, (b // 2) % 2, b % 2
    chunks, wide = buf.shape[0], buf.shape[5]
    group = dbuf.shape[3]
    blocks = chunks // group
    tokens = pooled.shape[0]
    half = tokens // 2
    piece = half // pieces
    tasks = tower_hidden.shape[0]
    experts = gate.shape[0]
    deep_rows = w_second.shape[1]
    width = w_third.shape[2]
    splits = w_second.shape[2] // width
    deep = chunks

    def at(zz, yy, cc):
        return zz * 4 + yy * 2 + cc

    across, sib = at(z, 1 - y, c), at(z, y, 1 - c)
    up, down = at(z + 1, y, c), at(z - 1, y, c)

    def remote(src, dst, send, recv, tt, bb):
        return pltpu.make_async_remote_copy(
            src_ref=src, dst_ref=dst, send_sem=send, recv_sem=recv,
            device_id=(tt, bb), device_id_type=MESH,
        )

    def shard(k, yy):
        cols = pl.ds(pl.multiple_of((k % blocks) * wide, 128), wide)
        return w_first.at[yy * group + k // blocks, :, cols]

    def own_copy(k):
        return pltpu.make_async_copy(shard(k, y), buf.at[k, z, y, c], loc.at[k])

    def deep_parts(yy):
        own = pl.ds(yy * group, group)
        to = dbuf.at[z, y, c]
        parts = [
            (w_second.at[own, :, pl.ds(h * width, width)],
             to.at[:, pl.ds(h * deep_rows, deep_rows)])
            for h in range(splits)
        ]
        return parts + [(w_third.at[own], to.at[:, pl.ds(splits * deep_rows, w_third.shape[1])])]

    deep_copies = [
        pltpu.make_async_copy(src, dst, loc_deep.at[n])
        for n, (src, dst) in enumerate(deep_parts(y))
    ]
    deep_across = [
        remote(src, dst, yd_s.at[n], yd_r.at[n], t, across)
        for n, (src, dst) in enumerate(deep_parts(1 - y))
    ]
    tok_copy = pltpu.make_async_copy(pooled, tok.at[pl.ds(0, tokens)], loc_tok.at[0])

    for copy in deep_copies:
        copy.start()

    @pl.loop(0, chunks)
    def _(k):
        own_copy(k).start()

    tok_copy.start()

    barrier = pltpu.get_barrier_semaphore()
    for tt, bb in (
        (t, across), (t, sib), (t, at((z + 1) % nz, y, c)), (t, at((z + nz - 1) % nz, y, c)),
        (1 - t, b), (1 - t, across),
    ):
        pl.semaphore_signal(barrier, inc=1, device_id=(tt, bb), device_id_type=MESH)
    pl.semaphore_wait(barrier, 6)

    def y_move(k):
        return remote(shard(k, 1 - y), buf.at[k, z, y, c], y_s.at[k], y_r.at[k], t, across)

    def tok_rows(h, p):
        return pl.ds(pl.multiple_of(h * half + p * piece, 16), piece)

    def p_move(p):
        rows = pl.ds(pl.multiple_of(tokens + t * half + p * piece, 16), piece)
        return remote(pooled.at[tok_rows(t, p)], tok.at[rows], p_s.at[p], p_r.at[p], t, across)

    def q_move(p):
        rows = pl.ds(pl.multiple_of(tokens + t * half + p * piece, 16), piece)
        return remote(tok.at[rows], tok.at[rows], q_s.at[p], q_r.at[p], 1 - t, b)

    swaps = [
        remote(gate, gate_rx, g_s.at[0], g_r.at[0], 1 - t, b),
        remote(tower_hidden, th_all.at[pl.ds(t * tasks, tasks)], g_s.at[1], g_r.at[1], 1 - t, b),
        remote(tower_out, to_all.at[t], g_s.at[2], g_r.at[2], 1 - t, b),
    ]

    for move in deep_across:
        move.start()
    y_move(0).start()
    y_move(1).start()
    for k in range(2, chunks):
        y_move(k).start()
    for p in range(pieces):
        p_move(p).start()
    for move in swaps:
        move.start()

    def pair(k, zz):
        if k is deep:
            return dbuf.at[zz, :, c]
        return buf.at[k, zz, :, c]

    def slot(k, yy):
        if k is deep:
            return dbuf.at[z, yy, c]
        return buf.at[k, z, yy, c]

    def row(k):
        return chunks if k is deep else k

    def z_own(k, yy, n, what):
        ref = slot(k, yy)

        @pl.when(z < nz - 1)
        def _():
            what(remote(ref, ref, up_s.at[row(k), n], z_r.at[row(k), z], t, up))

        @pl.when(z > 0)
        def _():
            what(remote(ref, ref, dn_s.at[row(k), n], z_r.at[row(k), z], t, down))

    def z_up(k, zz):
        return remote(pair(k, zz), pair(k, zz), up_s.at[row(k), zz], z_r.at[row(k), zz], t, up)

    def z_down(k, zz):
        return remote(pair(k, zz), pair(k, zz), dn_s.at[row(k), zz], z_r.at[row(k), zz], t, down)

    def sib_move(k, zz):
        return remote(pair(k, zz), pair(k, zz), sib_s.at[row(k), zz], sib_r.at[row(k), zz], t, sib)

    def start(copy):
        copy.start()

    def own_start(k):
        if k is deep:
            for copy in deep_copies:
                copy.wait()
        else:
            own_copy(k).wait()
        z_own(k, y, z, start)

    def own_finish(k):
        if k is deep:
            for move in deep_across:
                move.wait_recv()
        else:
            y_move(k).wait_recv()
        z_own(k, 1 - y, nz, start)
        sib_move(k, z).start()

    def z_step(k, d):
        @pl.when(z >= d)
        def _():
            z_up(k, z - d).wait_recv()

            @pl.when(z < nz - 1)
            def _():
                z_up(k, z - d).start()

            sib_move(k, z - d).start()

        @pl.when(z + d < nz)
        def _():
            z_down(k, z + d).wait_recv()

            @pl.when(z > 0)
            def _():
                z_down(k, z + d).start()

            sib_move(k, z + d).start()

    def sib_wait(k):
        @pl.loop(0, nz)
        def _(zz):
            sib_move(k, zz).wait_recv()

    ahead = 3
    own_start(deep)
    for k in range(ahead):
        own_start(k)
    own_finish(deep)
    for k in range(ahead):
        own_finish(k)
    for d in range(1, nz):
        z_step(deep, d)

    tok_copy.wait()
    for swap in swaps:
        swap.wait_recv()
    th_all[pl.ds(t * tasks, tasks)] = tower_hidden[...]
    to_all[t] = tower_out[...]
    for e in range(experts):
        n = gate.shape[1]
        gate_all[e * n : (e + 1) * n, :] = gate[e].astype(F32)
        gate_all[(experts + e) * n : (experts + e + 1) * n, :] = gate_rx[e].astype(F32)
    mine = pl.ds(pl.multiple_of(t * half, 16), half)
    wts[...] = jnp.exp(
        lax.dot_general(
            tok[mine, :], gate_all[...].astype(BF16), (((1,), (1,)), ((), ())),
            preferred_element_type=F32,
        )
    )
    acc[...] = jnp.zeros_like(acc)
    sib_wait(deep)

    def route(g):
        near = g // 2
        owner = t + (1 - g % 2) * (1 - 2 * t)
        bb = at(z, jnp.where(near == 1, y, 1 - y), c)
        return near, owner, bb

    def from_slot(owner, i):
        return (jnp.where(owner == t, 0, 1) * 2 + y) * group + i

    def o_move(i, g):
        near, owner, bb = route(g)
        n = from_slot(owner, i)
        return remote(out_tx.at[i, g], out_rx.at[n], o_s.at[i, g], o_r.at[n], owner, bb)

    def compute(k, g):
        near, owner, _ = route(g)
        rows = pl.ds(pl.multiple_of((1 - near) * tokens + owner * half, 16), half)
        cols = pl.ds(pl.multiple_of((k % blocks) * wide, 128), wide)
        weights = buf[k].reshape(-1, wide)
        first[rows, cols] = jnp.maximum(dot(tok[rows, :], weights), 0.0).astype(BF16)

        @pl.when(k % blocks == blocks - 1)
        def _():
            i = k // blocks
            hidden = first[rows, :]
            w3 = dbuf[:, :, :, i, pl.ds(splits * deep_rows, w_third.shape[1]), :].reshape(-1, width)
            total = None
            for h in range(splits):
                w2 = dbuf[:, :, :, i, pl.ds(h * deep_rows, deep_rows), :].reshape(-1, width)
                second = jnp.maximum(dot(hidden, w2), 0.0).astype(BF16)
                part = dot(second, w3[h * width : (h + 1) * width])
                total = part if total is None else total + part
            value = jnp.maximum(total, 0.0).astype(BF16)

            @pl.when(g < 3)
            def _():
                out_tx[i, g] = value
                o_move(i, g).start()

            @pl.when(g == 3)
            def _():
                out_rx[from_slot(t, i)] = value

    def accumulate(far, yy, i):
        value = out_rx[(far * 2 + yy) * group + i].astype(F32)
        n = gate.shape[1]
        for j in range(n):
            col = (far * experts + yy * group + i) * n + j
            acc[j] = acc[j] + wts[:, col : col + 1] * value

    def mix_in(i):
        for far in range(2):
            for yy in range(2):
                n = (far * 2 + yy) * group + i

                def waiting():
                    remote(out_tx.at[i, 0], out_rx.at[n], o_s.at[i, 0], o_r.at[n], t, across).wait_recv()

                if far == 0:
                    pl.when(y != yy)(waiting)
                else:
                    waiting()
                accumulate(far, yy, i)

    def lag(j):
        most = jnp.minimum(j + 1, jnp.maximum(0, 3 * (j - first_lag + 1)))
        return jnp.where(edge, most, 0)

    first_lag = 4
    edge = jnp.logical_or(z == 0, z == nz - 1)
    per = jnp.where(edge, -(-pieces // 3), -(-pieces // first_lag))

    @pl.loop(0, chunks)
    def _(i):
        @pl.when(i + ahead < chunks)
        def _():
            own_start(i + ahead)
            own_finish(i + ahead)

        @pl.when(i >= 1)
        def _():
            sib_wait(i - 1)
            compute(i - 1, 2)

        z_step(i, 1)

        @pl.when(i >= 1)
        def _():
            compute(i - 1, 3)

        for d in range(2, nz - 1):
            z_step(i, d)

        @pl.when(jnp.logical_and(edge, i == first_lag + 1))
        def _():
            @pl.loop(0, pieces)
            def _(p):
                q_move(p).wait_recv()

        @pl.when(i > first_lag)
        def _():
            @pl.loop(lag(i - 2), lag(i - 1))
            def _(k):
                compute(k, 0)
                compute(k, 1)

        z_step(i, nz - 1)

        @pl.when(jnp.logical_and(i >= 1, i <= first_lag))
        def _():
            @pl.loop(jnp.minimum((i - 1) * per, pieces), jnp.minimum(i * per, pieces))
            def _(p):
                p_move(p).wait_recv()
                q_move(p).start()

    last = chunks - 1

    @pl.when(jnp.logical_not(edge))
    def _():
        @pl.loop(0, pieces)
        def _(p):
            q_move(p).wait_recv()

    @pl.loop(lag(last - 1), last)
    def _(k):
        compute(k, 0)
        compute(k, 1)

    sib_wait(last)

    @pl.loop(0, 4)
    def _(g):
        compute(last, g)

    for i in range(group):
        mix_in(i)

    n = gate.shape[1]
    for j in range(n):
        total = None
        for e in range(2 * experts):
            w = wts[:, e * n + j : e * n + j + 1]
            total = w if total is None else total + w
        mix = (acc[j] / total).astype(BF16)
        tower = jnp.maximum(dot(mix, th_all[j]), 0.0).astype(BF16)
        vector = jnp.broadcast_to(to_all[j // tasks, j % tasks : j % tasks + 1, :], (16, tower.shape[1]))
        line = lax.dot_general(
            vector, tower, (((1,), (1,)), ((), ())), preferred_element_type=F32
        )
        res[j // tasks, j % tasks : j % tasks + 1, :] = line[:1]
    r_move = remote(res.at[1 - t], res_rx, r_s.at[0], r_r.at[0], 1 - t, b)
    r_move.start()
    out[:, pl.ds(pl.multiple_of(t * half, 128), half)] = res[t, 0:tasks, :]

    for move in deep_across:
        move.wait_send()
    for swap in swaps:
        swap.wait_send()

    @pl.loop(0, pieces)
    def _(p):
        p_move(p).wait_send()
        q_move(p).wait_send()

    for i in range(group):
        @pl.loop(0, 3)
        def _(g):
            o_move(i, g).wait_send()

    def sent(k):
        z_own(k, y, z, lambda copy: copy.wait_send())
        z_own(k, 1 - y, nz, lambda copy: copy.wait_send())

        @pl.loop(0, nz)
        def _(zz):
            sib_move(k, zz).wait_send()

            @pl.when(jnp.logical_and(z < nz - 1, zz < z))
            def _():
                z_up(k, zz).wait_send()

            @pl.when(jnp.logical_and(z > 0, zz > z))
            def _():
                z_down(k, zz).wait_send()

    sent(deep)

    @pl.loop(0, chunks)
    def _(k):
        y_move(k).wait_send()
        sent(k)

    r_move.wait()
    out[:, pl.ds(pl.multiple_of((1 - t) * half, 128), half)] = res_rx[0:tasks, :]


def fused(nb, pooled, gate_weight, w_first, w_second, w_third, tower_hidden, tower_out):
    tokens, width_in = pooled.shape
    experts, rows, h1 = w_first.shape
    tasks = tower_hidden.shape[0]
    all_tasks = gate_weight.shape[2]
    deep_rows, deep_width = w_second.shape[1:]
    last_rows, last_width = w_third.shape[1:]
    nz = nb // 4
    group = experts // 2
    wide = h1 // BLOCKS
    chunks = group * BLOCKS
    half = tokens // 2
    splits = deep_width // last_width
    packed_rows = splits * deep_rows + last_rows
    dma = pltpu.SemaphoreType.DMA
    vmem = pl.BlockSpec(memory_space=pltpu.VMEM)
    anywhere = pl.BlockSpec(memory_space=pl.ANY)
    gate = jnp.transpose(gate_weight, (1, 2, 0))
    lines = pl.pallas_call(
        functools.partial(fused_kernel, nb, PIECES),
        out_shape=jax.ShapeDtypeStruct((tasks, tokens), F32),
        in_specs=[anywhere, vmem, anywhere, anywhere, anywhere, vmem, vmem],
        out_specs=vmem,
        scratch_shapes=[
            pltpu.VMEM((2 * tokens, width_in), BF16),
            pltpu.VMEM((chunks, nz, 2, 2, rows, wide), BF16),
            pltpu.VMEM((nz, 2, 2, group, packed_rows, last_width), BF16),
            pltpu.VMEM((2 * tokens, h1), BF16),
            pltpu.VMEM((group, 3, half, last_width), BF16),
            pltpu.VMEM((4 * group, half, last_width), BF16),
            pltpu.VMEM(gate.shape, BF16),
            pltpu.VMEM((2 * experts * all_tasks, width_in), F32),
            pltpu.VMEM((half, 2 * experts * all_tasks), F32),
            pltpu.VMEM((all_tasks, half, last_width), F32),
            pltpu.VMEM((all_tasks,) + tower_hidden.shape[1:], BF16),
            pltpu.VMEM((2,) + tower_out.shape, BF16),
            pltpu.VMEM((2, 8, half), F32),
            pltpu.VMEM((8, half), F32),
            dma((chunks,)),
            dma((splits + 1,)),
            dma((1,)),
            dma((chunks,)),
            dma((chunks,)),
            dma((splits + 1,)),
            dma((splits + 1,)),
            dma((PIECES,)),
            dma((PIECES,)),
            dma((PIECES,)),
            dma((PIECES,)),
            dma((3,)),
            dma((3,)),
            dma((chunks + 1, nz)),
            dma((chunks + 1, nz + 1)),
            dma((chunks + 1, nz + 1)),
            dma((chunks + 1, nz)),
            dma((chunks + 1, nz)),
            dma((group, 3)),
            dma((4 * group,)),
            dma((1,)),
            dma((1,)),
        ],
        compiler_params=pltpu.CompilerParams(
            collective_id=0, has_side_effects=True, vmem_limit_bytes=VMEM_BYTES
        ),
    )(pooled, gate, w_first, w_second, w_third, tower_hidden, tower_out)
    return lines.T


def gathered_first(pooled, gate_weight, w_first, w_second, w_third, tower_hidden, tower_out):
    tok_rows = pooled.shape[0]
    width_in = pooled.shape[1]
    local_experts = w_first.shape[0]
    all_tasks = gate_weight.shape[2]
    own_tasks = tower_hidden.shape[0]
    gathered = lax.all_gather(w_first, "batch", axis=1, tiled=True)
    deep_rows, deep_width = w_second.shape[1], w_second.shape[2]
    last_rows, last_width = w_third.shape[1], w_third.shape[2]
    halves = deep_width // last_width
    packed = jnp.concatenate(
        [w_second[:, :, i * last_width : (i + 1) * last_width] for i in range(halves)] + [w_third],
        axis=1,
    )
    gathered, packed = lax.optimization_barrier((gathered, packed))
    packed = lax.all_gather(packed, "batch", axis=1, tiled=False)
    second_all = jnp.concatenate(
        [packed[:, :, i * deep_rows : (i + 1) * deep_rows] for i in range(halves)], axis=3
    ).reshape(local_experts, -1, deep_width)
    third_all = packed[:, :, halves * deep_rows :].reshape(local_experts, -1, last_width)
    summed = jnp.einsum("tr,erh->eth", pooled, gathered, preferred_element_type=jnp.float32)
    first = jax.nn.relu(summed).astype(jnp.bfloat16)
    logits = jnp.dot(
        pooled,
        gate_weight.reshape(width_in, local_experts * all_tasks),
        preferred_element_type=jnp.float32,
    )
    weights = jnp.exp(logits.reshape(tok_rows, local_experts, all_tasks))
    gate_total = jnp.sum(weights, axis=1)
    columns = first
    second = jax.nn.relu(
        jnp.einsum(
            "etr,erh->eth",
            columns,
            second_all,
            preferred_element_type=jnp.float32,
        )
    ).astype(jnp.bfloat16)
    columns = second
    expert_out = jax.nn.relu(
        jnp.einsum(
            "etr,erh->eth",
            columns,
            third_all,
            preferred_element_type=jnp.float32,
        )
    ).astype(jnp.bfloat16)
    numer = jnp.einsum("tek,eth->tkh", weights, expert_out.astype(jnp.float32))
    groups = all_tasks // own_tasks
    me = lax.axis_index("task")
    numer_own = lax.dynamic_slice_in_dim(numer, me * own_tasks, own_tasks, 1)
    total_own = lax.dynamic_slice_in_dim(gate_total, me * own_tasks, own_tasks, 1)
    for shift in range(1, groups):
        ring = [(i, (i + shift) % groups) for i in range(groups)]
        other = lax.rem(me + shift, groups) * own_tasks
        numer_sent = lax.dynamic_slice_in_dim(numer, other, own_tasks, 1).astype(jnp.bfloat16)
        total_sent = lax.dynamic_slice_in_dim(gate_total, other, own_tasks, 1)
        numer_own = numer_own + lax.ppermute(numer_sent, "task", ring).astype(jnp.float32)
        total_own = total_own + lax.ppermute(total_sent, "task", ring)
    mix = (numer_own / total_own[:, :, None]).astype(jnp.bfloat16)
    tower = jax.nn.relu(
        jnp.einsum("tkh,khm->tkm", mix, tower_hidden, preferred_element_type=jnp.float32)
    ).astype(jnp.bfloat16)
    return jnp.einsum("tkm,km->tk", tower, tower_out, preferred_element_type=jnp.float32)


def fits(mesh, pooled, gate_weight, w_first, w_second, w_third):
    even = all(w.shape[1] % 16 == 0 for w in (w_first, w_second, w_third))
    tokens, experts = pooled.shape[0], w_first.shape[0]
    cut = tokens % (32 * PIECES) == 0 and tokens % 256 == 0 and experts % 2 == 0
    lanes = w_first.shape[2] % (128 * BLOCKS) == 0 and w_second.shape[2] % w_third.shape[2] == 0
    wanted = (gate_weight.shape[1] * gate_weight.shape[2]) <= 64
    two = mesh.shape["task"] == 2 and gate_weight.shape[2] % 2 == 0
    return even and cut and lanes and wanted and two and mesh.shape["batch"] % 4 == 0


def solution(mesh):
    placed = (
        P("batch", None),
        P(None, "task", None),
        P("task", "batch", None),
        P("task", "batch", None),
        P("task", "batch", None),
        P("task", None, None),
        P("task", None),
    )

    def per_device(*args):
        if fits(mesh, *args[:5]):
            return fused(mesh.shape["batch"], *args)
        return gathered_first(*args)

    return jax.shard_map(
        per_device, mesh=mesh, in_specs=placed, out_specs=P("batch", "task"), check_vma=False
    )
```

```python
import functools

import jax
import jax.numpy as jnp
from jax import lax
from jax.experimental import pallas as pl
from jax.experimental.pallas import tpu as pltpu
from jax.sharding import PartitionSpec as P

MESH = pl.DeviceIdType.MESH
BF16, F32 = jnp.bfloat16, jnp.float32
VMEM_BYTES = 63 * 1024 * 1024
BLOCKS, PIECES = 4, 12
SPOTS = (3, 6, 9, 11)
OWN_AHEAD, OWN_AHEAD_EDGE, PAIR_AHEAD, FEED_AHEAD = 5, 3, 4, 1
NEAR_AHEAD, NEAR_AHEAD_EDGE = 3, 3
CROSS_LAG, CROSS_LAG_EDGE, WORK_LAG, WORK_LAG_EDGE = 2, 2, 3, 4
PIECE_LAG, PASS_LAG = 2, 1
FAR_STEPS = (14, 16)


def dot(a, b):
    return jnp.dot(a, b, preferred_element_type=F32)


def fused_kernel(
    nb, pieces,
    pooled, gate, w_first, w_second, w_third, tower_hidden, tower_out, out,
    tok, buf, dbuf, first, out_tx, out_rx, gate_rx, gate_all, wts, acc, th_all, to_all, res, res_rx,
    loc, loc_deep, loc_tok, p_s, p_r, q_s, q_r, g_s, g_r,
    got, z_s, y_s, f_s, sib_r, sib_s, o_s, o_r, far_s, far_r, r_s, r_r,
):
    t, b = lax.axis_index("task"), lax.axis_index("batch")
    nz = nb // 4
    z, y, c = b // 4, (b // 2) % 2, b % 2
    high = z // (nz // 2)
    edge = jnp.logical_or(z == 0, z == nz - 1)
    inner = jnp.logical_not(edge)
    zp = jnp.where(edge, z + 1 - 2 * high, z - 1 + 2 * high)
    zm = nz - 1 - z
    zq = nz - 1 - zp
    chunks, wide = buf.shape[0], buf.shape[5]
    experts = dbuf.shape[0]
    blocks = chunks // experts
    tokens = pooled.shape[0]
    half = tokens // 2
    piece = half // pieces
    tasks = tower_hidden.shape[0]
    deep_rows = w_second.shape[1]
    width = w_third.shape[2]
    splits = w_second.shape[2] // width

    def at(zz, yy, cc):
        return zz * 4 + yy * 2 + cc

    across, sib = at(z, 1 - y, c), at(z, y, 1 - c)

    def both(p, q):
        return jnp.logical_and(p, q)

    def either(p, q):
        return jnp.logical_or(p, q)

    def remote(src, dst, send, recv, tt, bb):
        return pltpu.make_async_remote_copy(
            src_ref=src, dst_ref=dst, send_sem=send, recv_sem=recv,
            device_id=(tt, bb), device_id_type=MESH,
        )

    def passed(n):
        count = 0
        for spot in SPOTS:
            count = count + jnp.where(n > spot, 1, 0)
        return count

    def zeroth(n):
        hit = n == SPOTS[0]
        for spot in SPOTS[1:]:
            hit = either(hit, n == spot)
        return hit

    def rank(n):
        return n - passed(n)

    def expert(n):
        return jnp.where(zeroth(n), 0, 1 + rank(n) // blocks)

    def block(n):
        return jnp.where(zeroth(n), passed(n), rank(n) % blocks)

    def own_copy(n):
        cols = pl.ds(pl.multiple_of(block(n) * wide, 128), wide)
        return pltpu.make_async_copy(
            w_first.at[expert(n), :, cols], buf.at[n, z, y, c], loc.at[n]
        )

    deep_copies = [
        pltpu.make_async_copy(
            w_second.at[:, :, pl.ds(h * width, width)],
            dbuf.at[:, z, y, c, pl.ds(h * deep_rows, deep_rows)], loc_deep.at[h],
        )
        for h in range(splits)
    ] + [
        pltpu.make_async_copy(
            w_third, dbuf.at[:, z, y, c, pl.ds(splits * deep_rows, w_third.shape[1])],
            loc_deep.at[splits],
        )
    ]
    tok_copy = pltpu.make_async_copy(pooled, tok.at[pl.ds(0, tokens)], loc_tok.at[0])

    for copy in deep_copies:
        copy.start()

    @pl.loop(0, chunks)
    def _(n):
        own_copy(n).start()

    tok_copy.start()

    barrier = pltpu.get_barrier_semaphore()
    for tt, bb in (
        (t, across), (t, sib), (t, at(zp, y, c)), (t, at(zm, y, c)), (1 - t, b),
        (1 - t, at(zp, y, c)),
    ):
        pl.semaphore_signal(barrier, inc=1, device_id=(tt, bb), device_id_type=MESH)
    pl.semaphore_wait(barrier, 6)

    swaps = [
        remote(gate, gate_rx, g_s.at[0], g_r.at[0], 1 - t, b),
        remote(tower_hidden, th_all.at[pl.ds(t * tasks, tasks)], g_s.at[1], g_r.at[1], 1 - t, b),
        remote(tower_out, to_all.at[t], g_s.at[2], g_r.at[2], 1 - t, b),
    ]
    for move in swaps:
        move.start()

    def chunk(n):
        return (lambda zz, yy: buf.at[n, zz, yy, c], lambda zz: buf.at[n, zz, :, c],
                n, zeroth(n), jnp.logical_not(zeroth(n)))

    def deep(e):
        return (lambda zz, yy: dbuf.at[e, zz, yy, c], lambda zz: dbuf.at[e, zz, :, c],
                chunks + e, e >= 0, e != 0)

    def hop(it, zz, yy, sem, bb):
        ref = it[0](zz, yy)
        return remote(ref, ref, sem, got.at[it[2], zz, yy], t, bb)

    def to_mid(it, zz, yy, key):
        return hop(it, zz, yy, z_s.at[it[2], key], at(zm, y, c))

    def to_pair(it, zz, yy, key):
        return hop(it, zz, yy, f_s.at[it[2], key], at(zp, y, c))

    def to_side(it, zz):
        return hop(it, zz, y, y_s.at[it[2], zz], across)

    def to_sib(it, zz):
        ref = it[1](zz)
        return remote(ref, ref, sib_s.at[it[2], zz], sib_r.at[it[2], zz], t, sib)

    def landed(it, zz, yy):
        to_pair(it, zz, yy, 0).wait_recv()

    def own(it):
        _, _, _, dup, ends = it
        to_side(it, z).start()

        @pl.when(inner)
        def _():
            to_mid(it, z, y, 0).start()

        @pl.when(either(edge, ends))
        def _():
            to_pair(it, z, y, 0).start()

    def finish(it):
        _, _, _, dup, ends = it
        landed(it, z, 1 - y)

        @pl.when(both(dup, inner))
        def _():
            to_mid(it, z, 1 - y, 1).start()

        @pl.when(both(dup, either(edge, ends)))
        def _():
            to_pair(it, z, 1 - y, 1).start()

        @pl.when(either(inner, ends))
        def _():
            to_sib(it, z).start()

    def feed(it):
        _, _, _, dup, ends = it
        landed(it, zp, y)
        to_mid(it, zp, y, 2).start()

        @pl.when(dup)
        def _():
            landed(it, zp, 1 - y)
            to_mid(it, zp, 1 - y, 3).start()
            to_sib(it, zp).start()

        @pl.when(jnp.logical_not(dup))
        def _():
            to_side(it, zp).start()

    def take(it, key, zz):
        _, _, _, dup, ends = it
        landed(it, zz, y)

        @pl.when(both(inner, ends))
        def _():
            to_pair(it, zz, y, key).start()

        @pl.when(dup)
        def _():
            landed(it, zz, 1 - y)

            @pl.when(both(inner, ends))
            def _():
                to_pair(it, zz, 1 - y, key + 1).start()

            to_sib(it, zz).start()

        @pl.when(jnp.logical_not(dup))
        def _():
            to_side(it, zz).start()

    def near(it):
        @pl.when(either(inner, it[4]))
        def _():
            take(it, 2, jnp.where(inner, zm, zp))

    def far(it):
        @pl.when(either(inner, it[4]))
        def _():
            take(it, 4, zq)

        @pl.when(both(edge, it[4]))
        def _():
            take(it, 2, zm)

    def cross(it):
        @pl.when(jnp.logical_not(it[3]))
        def _():
            for zz in (zp, zm, zq):
                landed(it, zz, 1 - y)
                to_sib(it, zz).start()

    def sib_wait(it):
        @pl.loop(0, nz)
        def _(zz):
            to_sib(it, zz).wait_recv()

    def stage(n, step):
        @pl.when(block(n) == 2)
        def _():
            step(deep(expert(n)))

        step(chunk(n))

    def own_at(n):
        own_copy(n).wait()
        stage(n, own)

    def tok_rows(h, p):
        return pl.ds(pl.multiple_of(h * half + p * piece, 16), piece)

    def far_rows(p):
        return pl.ds(pl.multiple_of(tokens + t * half + p * piece, 16), piece)

    def p_move(p):
        return remote(
            pooled.at[tok_rows(t, p)], tok.at[far_rows(p)], p_s.at[p], p_r.at[p], t, at(zp, y, c)
        )

    def q_move(p):
        rows = far_rows(p)
        return remote(tok.at[rows], tok.at[rows], q_s.at[p], q_r.at[p], 1 - t, b)

    for copy in deep_copies:
        copy.wait()
    own_ahead = jnp.where(edge, OWN_AHEAD_EDGE, OWN_AHEAD)

    @pl.loop(0, own_ahead)
    def _(n):
        own_at(n)

    @pl.when(edge)
    def _():
        @pl.loop(0, chunks)
        def _(n):
            @pl.when(n + OWN_AHEAD_EDGE < chunks)
            def _():
                own_at(n + OWN_AHEAD_EDGE)

            stage(n, finish)

            @pl.when(both(n > PIECE_LAG, n <= PIECE_LAG + pieces))
            def _():
                p_move(n - PIECE_LAG - 1).start()

    @pl.when(inner)
    def _():
        @pl.loop(0, PAIR_AHEAD)
        def _(n):
            stage(n, finish)

        @pl.loop(0, FEED_AHEAD)
        def _(n):
            stage(n, feed)

    tok_copy.wait()
    for swap in swaps:
        swap.wait_recv()
    th_all[pl.ds(t * tasks, tasks)] = tower_hidden[...]
    to_all[t] = tower_out[...]
    every = gate.shape[1]
    for e in range(experts):
        gate_all[e * every : (e + 1) * every, :] = gate[e].astype(F32)
        gate_all[(experts + e) * every : (experts + e + 1) * every, :] = gate_rx[e].astype(F32)
    mine = pl.ds(pl.multiple_of(t * half, 16), half)
    raw = jnp.exp(
        lax.dot_general(
            tok[mine, :], gate_all[...].astype(BF16), (((1,), (1,)), ((), ())),
            preferred_element_type=F32,
        )
    )
    lane = lax.broadcasted_iota(jnp.int32, raw.shape, 1)
    below = jnp.ones_like(raw)
    for j in range(every):
        own_task = lane % every == j
        total = jnp.sum(jnp.where(own_task, raw, 0.0), axis=1, keepdims=True)
        below = jnp.where(own_task, total, below)
    wts[...] = raw / below
    acc[...] = jnp.zeros_like(acc)

    def o_move(e):
        slot = experts + e
        return remote(out_tx.at[e], out_rx.at[slot], o_s.at[e], o_r.at[slot], 1 - t, b)

    def narrow(e, hidden):
        w3 = dbuf[e, :, :, :, pl.ds(splits * deep_rows, w_third.shape[1]), :].reshape(-1, width)
        total = None
        for h in range(splits):
            w2 = dbuf[e, :, :, :, pl.ds(h * deep_rows, deep_rows), :].reshape(-1, width)
            second = jnp.maximum(dot(hidden, w2), 0.0).astype(BF16)
            part = dot(second, w3[h * width : (h + 1) * width])
            total = part if total is None else total + part
        return jnp.maximum(total, 0.0).astype(BF16)

    def widen(n, rows, kept):
        cols = pl.ds(pl.multiple_of(block(n) * wide, 128), wide)
        weights = buf[n].reshape(-1, wide)
        first[kept, cols] = jnp.maximum(dot(tok[rows, :], weights), 0.0).astype(BF16)

    def compute(n, g):
        owner = 1 - t if g == 0 else t
        base = jnp.where(zeroth(n), 0, 2 * tokens)
        rows = pl.ds(pl.multiple_of(owner * half, 16), half)
        kept = pl.ds(pl.multiple_of(base + owner * half, 16), half)
        widen(n, rows, kept)

        @pl.when(block(n) == blocks - 1)
        def _():
            e = expert(n)
            value = narrow(e, first[kept, :])
            if g == 0:
                out_tx[e] = value
                o_move(e).start()
            else:
                out_rx[e] = value

    part = half // 2

    def far_move(f, side):
        owner = t + (1 - side) * (1 - 2 * t)
        rows = pl.ds(pl.multiple_of(f * part, 16), part)
        return remote(
            out_tx.at[experts + side, rows], out_rx.at[(1 - side) * experts, rows],
            far_s.at[side, f], far_r.at[1 - side, f], owner, at(zp, y, c),
        )

    def compute_far(f, side):
        owner = t + (1 - side) * (1 - 2 * t)
        rows = pl.ds(pl.multiple_of(tokens + owner * half + f * part, 16), part)

        @pl.loop(0, blocks)
        def _(s):
            spot = SPOTS[0]
            for k in range(1, blocks):
                spot = jnp.where(s == k, SPOTS[k], spot)
            widen(spot, rows, rows)

        there = pl.ds(pl.multiple_of(f * part, 16), part)
        out_tx[experts + side, there, :] = narrow(0, first[rows, :])
        far_move(f, side).start()

    near_ahead = jnp.where(edge, NEAR_AHEAD_EDGE, NEAR_AHEAD)

    @pl.loop(0, near_ahead)
    def _(n):
        stage(n, near)

    cross_lag = jnp.where(edge, CROSS_LAG_EDGE, CROSS_LAG)
    work_lag = jnp.where(edge, WORK_LAG_EDGE, WORK_LAG)

    @pl.loop(0, chunks + max(WORK_LAG, WORK_LAG_EDGE))
    def _(i):
        @pl.when(inner)
        def _():
            @pl.when(i + OWN_AHEAD < chunks)
            def _():
                own_at(i + OWN_AHEAD)

            @pl.when(i + PAIR_AHEAD < chunks)
            def _():
                stage(i + PAIR_AHEAD, finish)

            @pl.when(i + FEED_AHEAD < chunks)
            def _():
                stage(i + FEED_AHEAD, feed)

        n = i - work_lag
        ready = both(both(n >= 0, n < chunks), either(inner, jnp.logical_not(zeroth(n))))

        @pl.when(ready)
        def _():
            stage(n, sib_wait)
            compute(n, 0)

        @pl.when(i + near_ahead < chunks)
        def _():
            stage(i + near_ahead, near)

        @pl.when(i < chunks)
        def _():
            stage(i, far)

        @pl.when(ready)
        def _():
            compute(n, 1)

        k = i - cross_lag

        @pl.when(both(k >= 0, k < chunks))
        def _():
            stage(k, cross)

        @pl.when(both(inner, both(i > PASS_LAG, i <= PASS_LAG + pieces)))
        def _():
            p_move(i - PASS_LAG - 1).wait_recv()
            q_move(i - PASS_LAG - 1).start()

        for f in range(2):
            @pl.when(both(inner, i == FAR_STEPS[f]))
            def _():
                @pl.loop(f * pieces // 2, (f + 1) * pieces // 2)
                def _(p):
                    q_move(p).wait_recv()

        first_far = both(i >= FAR_STEPS[0], i < FAR_STEPS[0] + 2)
        second_far = both(i >= FAR_STEPS[1], i < FAR_STEPS[1] + 2)

        @pl.when(both(inner, either(first_far, second_far)))
        def _():
            f = jnp.where(i >= FAR_STEPS[1], 1, 0)
            compute_far(f, i - jnp.where(f == 1, FAR_STEPS[1], FAR_STEPS[0]))

    def accumulate(far, e):
        value = out_rx[far * experts + e].astype(F32)
        for j in range(every):
            col = (far * experts + e) * every + j
            acc[j] = acc[j] + wts[:, col : col + 1] * value

    def waiting(e):
        o_move(e).wait_recv()

    def waiting_far(far):
        for f in range(2):
            far_move(f, 1 - far).wait_recv()

    for e in range(1, experts):
        accumulate(0, e)
    for e in range(1, experts - 1):
        waiting(e)
        accumulate(1, e)
    pl.when(edge)(lambda: waiting_far(0))
    accumulate(0, 0)
    pl.when(edge)(lambda: waiting_far(1))
    pl.when(inner)(lambda: waiting(0))
    accumulate(1, 0)
    for swap in swaps:
        swap.wait_send()

    @pl.when(edge)
    def _():
        @pl.loop(0, pieces)
        def _(p):
            p_move(p).wait_send()

    @pl.when(inner)
    def _():
        @pl.loop(0, pieces)
        def _(p):
            q_move(p).wait_send()

        o_move(0).wait_send()
        for f in range(2):
            for side in range(2):
                far_move(f, side).wait_send()

    @pl.loop(1, experts)
    def _(e):
        o_move(e).wait_send()

    def sent(it):
        _, _, _, dup, ends = it
        to_side(it, z).wait_send()

        @pl.when(inner)
        def _():
            to_mid(it, z, y, 0).wait_send()
            to_mid(it, zp, y, 2).wait_send()

            @pl.when(dup)
            def _():
                to_mid(it, z, 1 - y, 1).wait_send()
                to_mid(it, zp, 1 - y, 3).wait_send()

            @pl.when(ends)
            def _():
                to_pair(it, zm, y, 2).wait_send()
                to_pair(it, zq, y, 4).wait_send()

                @pl.when(dup)
                def _():
                    to_pair(it, zm, 1 - y, 3).wait_send()
                    to_pair(it, zq, 1 - y, 5).wait_send()

        @pl.when(either(edge, ends))
        def _():
            to_pair(it, z, y, 0).wait_send()

            @pl.when(dup)
            def _():
                to_pair(it, z, 1 - y, 1).wait_send()

        @pl.when(jnp.logical_not(dup))
        def _():
            for zz in (zp, zm, zq):
                to_side(it, zz).wait_send()

        @pl.when(either(inner, ends))
        def _():
            @pl.loop(0, nz)
            def _(zz):
                to_sib(it, zz).wait_send()

    @pl.loop(0, chunks)
    def _(n):
        sent(chunk(n))

    @pl.loop(0, experts)
    def _(e):
        sent(deep(e))

    waiting(experts - 1)
    accumulate(1, experts - 1)

    for j in range(every):
        mix = acc[j].astype(BF16)
        tower = jnp.maximum(dot(mix, th_all[j]), 0.0).astype(BF16)
        vector = jnp.broadcast_to(to_all[j // tasks, j % tasks : j % tasks + 1, :], (16, tower.shape[1]))
        line = lax.dot_general(
            vector, tower, (((1,), (1,)), ((), ())), preferred_element_type=F32
        )
        res[j // tasks, j % tasks : j % tasks + 1, :] = line[:1]
    r_move = remote(res.at[1 - t], res_rx, r_s.at[0], r_r.at[0], 1 - t, b)
    r_move.start()
    out[:, pl.ds(pl.multiple_of(t * half, 128), half)] = res[t, 0:tasks, :]

    r_move.wait()
    out[:, pl.ds(pl.multiple_of((1 - t) * half, 128), half)] = res_rx[0:tasks, :]


def fused(nb, pooled, gate_weight, w_first, w_second, w_third, tower_hidden, tower_out):
    tokens, width_in = pooled.shape
    experts, rows, h1 = w_first.shape
    tasks = tower_hidden.shape[0]
    all_tasks = gate_weight.shape[2]
    deep_rows, deep_width = w_second.shape[1:]
    last_rows, last_width = w_third.shape[1:]
    nz = nb // 4
    wide = h1 // BLOCKS
    chunks = experts * BLOCKS
    items = chunks + experts
    half = tokens // 2
    splits = deep_width // last_width
    packed_rows = splits * deep_rows + last_rows
    dma = pltpu.SemaphoreType.DMA
    vmem = pl.BlockSpec(memory_space=pltpu.VMEM)
    anywhere = pl.BlockSpec(memory_space=pl.ANY)
    gate = jnp.transpose(gate_weight, (1, 2, 0))
    lines = pl.pallas_call(
        functools.partial(fused_kernel, nb, PIECES),
        out_shape=jax.ShapeDtypeStruct((tasks, tokens), F32),
        in_specs=[anywhere, vmem, anywhere, anywhere, anywhere, vmem, vmem],
        out_specs=vmem,
        scratch_shapes=[
            pltpu.VMEM((2 * tokens, width_in), BF16),
            pltpu.VMEM((chunks, nz, 2, 2, rows, wide), BF16),
            pltpu.VMEM((experts, nz, 2, 2, packed_rows, last_width), BF16),
            pltpu.VMEM((3 * tokens, h1), BF16),
            pltpu.VMEM((experts + 2, half, last_width), BF16),
            pltpu.VMEM((2 * experts, half, last_width), BF16),
            pltpu.VMEM(gate.shape, BF16),
            pltpu.VMEM((2 * experts * all_tasks, width_in), F32),
            pltpu.VMEM((half, 2 * experts * all_tasks), F32),
            pltpu.VMEM((all_tasks, half, last_width), F32),
            pltpu.VMEM((all_tasks,) + tower_hidden.shape[1:], BF16),
            pltpu.VMEM((2,) + tower_out.shape, BF16),
            pltpu.VMEM((2, 8, half), F32),
            pltpu.VMEM((8, half), F32),
            dma((chunks,)),
            dma((splits + 1,)),
            dma((1,)),
            dma((PIECES,)),
            dma((PIECES,)),
            dma((PIECES,)),
            dma((PIECES,)),
            dma((3,)),
            dma((3,)),
            dma((items, nz, 2)),
            dma((items, 4)),
            dma((items, nz)),
            dma((items, 6)),
            dma((items, nz)),
            dma((items, nz)),
            dma((experts,)),
            dma((2 * experts,)),
            dma((2, 2)),
            dma((2, 2)),
            dma((1,)),
            dma((1,)),
        ],
        compiler_params=pltpu.CompilerParams(
            collective_id=0, has_side_effects=True, vmem_limit_bytes=VMEM_BYTES
        ),
    )(pooled, gate, w_first, w_second, w_third, tower_hidden, tower_out)
    return lines.T


def gathered_first(pooled, gate_weight, w_first, w_second, w_third, tower_hidden, tower_out):
    tok_rows = pooled.shape[0]
    width_in = pooled.shape[1]
    local_experts = w_first.shape[0]
    all_tasks = gate_weight.shape[2]
    own_tasks = tower_hidden.shape[0]
    gathered = lax.all_gather(w_first, "batch", axis=1, tiled=True)
    deep_rows, deep_width = w_second.shape[1], w_second.shape[2]
    last_rows, last_width = w_third.shape[1], w_third.shape[2]
    halves = deep_width // last_width
    packed = jnp.concatenate(
        [w_second[:, :, i * last_width : (i + 1) * last_width] for i in range(halves)] + [w_third],
        axis=1,
    )
    gathered, packed = lax.optimization_barrier((gathered, packed))
    packed = lax.all_gather(packed, "batch", axis=1, tiled=False)
    second_all = jnp.concatenate(
        [packed[:, :, i * deep_rows : (i + 1) * deep_rows] for i in range(halves)], axis=3
    ).reshape(local_experts, -1, deep_width)
    third_all = packed[:, :, halves * deep_rows :].reshape(local_experts, -1, last_width)
    summed = jnp.einsum("tr,erh->eth", pooled, gathered, preferred_element_type=jnp.float32)
    first = jax.nn.relu(summed).astype(jnp.bfloat16)
    logits = jnp.dot(
        pooled,
        gate_weight.reshape(width_in, local_experts * all_tasks),
        preferred_element_type=jnp.float32,
    )
    weights = jnp.exp(logits.reshape(tok_rows, local_experts, all_tasks))
    gate_total = jnp.sum(weights, axis=1)
    columns = first
    second = jax.nn.relu(
        jnp.einsum(
            "etr,erh->eth",
            columns,
            second_all,
            preferred_element_type=jnp.float32,
        )
    ).astype(jnp.bfloat16)
    columns = second
    expert_out = jax.nn.relu(
        jnp.einsum(
            "etr,erh->eth",
            columns,
            third_all,
            preferred_element_type=jnp.float32,
        )
    ).astype(jnp.bfloat16)
    numer = jnp.einsum("tek,eth->tkh", weights, expert_out.astype(jnp.float32))
    groups = all_tasks // own_tasks
    me = lax.axis_index("task")
    numer_own = lax.dynamic_slice_in_dim(numer, me * own_tasks, own_tasks, 1)
    total_own = lax.dynamic_slice_in_dim(gate_total, me * own_tasks, own_tasks, 1)
    for shift in range(1, groups):
        ring = [(i, (i + shift) % groups) for i in range(groups)]
        other = lax.rem(me + shift, groups) * own_tasks
        numer_sent = lax.dynamic_slice_in_dim(numer, other, own_tasks, 1).astype(jnp.bfloat16)
        total_sent = lax.dynamic_slice_in_dim(gate_total, other, own_tasks, 1)
        numer_own = numer_own + lax.ppermute(numer_sent, "task", ring).astype(jnp.float32)
        total_own = total_own + lax.ppermute(total_sent, "task", ring)
    mix = (numer_own / total_own[:, :, None]).astype(jnp.bfloat16)
    tower = jax.nn.relu(
        jnp.einsum("tkh,khm->tkm", mix, tower_hidden, preferred_element_type=jnp.float32)
    ).astype(jnp.bfloat16)
    return jnp.einsum("tkm,km->tk", tower, tower_out, preferred_element_type=jnp.float32)


def fits(mesh, pooled, gate_weight, w_first, w_second, w_third):
    even = all(w.shape[1] % 16 == 0 for w in (w_first, w_second, w_third))
    tokens, experts = pooled.shape[0], w_first.shape[0]
    cut = tokens % (32 * PIECES) == 0 and tokens % 256 == 0 and experts >= 4
    lanes = w_first.shape[2] % (128 * BLOCKS) == 0 and w_second.shape[2] % w_third.shape[2] == 0
    wanted = (gate_weight.shape[1] * gate_weight.shape[2]) <= 64
    two = mesh.shape["task"] == 2 and gate_weight.shape[2] % 2 == 0
    held = (experts * (w_first.shape[1] * w_first.shape[2]) + tokens * pooled.shape[1] // 8) * 32
    return even and cut and lanes and wanted and two and mesh.shape["batch"] == 16 and held < 2**26


def solution(mesh):
    placed = (
        P("batch", None),
        P(None, "task", None),
        P("task", "batch", None),
        P("task", "batch", None),
        P("task", "batch", None),
        P("task", None, None),
        P("task", None),
    )

    def per_device(*args):
        if fits(mesh, *args[:5]):
            return fused(mesh.shape["batch"], *args)
        return gathered_first(*args)

    return jax.shard_map(
        per_device, mesh=mesh, in_specs=placed, out_specs=P("batch", "task"), check_vma=False
    )
```

```python
import functools

import jax
import jax.numpy as jnp
from jax import lax
from jax.experimental import pallas as pl
from jax.experimental.pallas import tpu as pltpu
from jax.sharding import PartitionSpec as P

MESH = pl.DeviceIdType.MESH
BF16, F32 = jnp.bfloat16, jnp.float32
VMEM_BYTES = 63 * 1024 * 1024
BLOCKS, PIECES = 4, 12
SPOTS = (3, 6, 9, 11)
OWN_AHEAD, OWN_AHEAD_EDGE, PAIR_AHEAD, FEED_AHEAD = 5, 3, 4, 1
NEAR_AHEAD, NEAR_AHEAD_EDGE = 3, 3
CROSS_LAG, CROSS_LAG_EDGE, WORK_LAG, WORK_LAG_EDGE = 2, 2, 3, 4
PIECE_LAG, PASS_LAG = 2, 1
FAR_STEPS = (14, 16)


def dot(a, b):
    return jnp.dot(a, b, preferred_element_type=F32)


def fused_kernel(
    nb, pieces,
    pooled, gate, w_first, w_second, w_third, tower_hidden, tower_out, out,
    tok, buf, dbuf, first, out_tx, out_rx, gate_rx, gate_all, wts, acc, th_all, to_all, res, res_rx,
    loc, loc_deep, loc_tok, p_s, p_r, q_s, q_r, g_s, g_r,
    got, z_s, y_s, f_s, sib_r, sib_s, o_s, o_r, far_s, far_r, r_s, r_r,
):
    t, b = lax.axis_index("task"), lax.axis_index("batch")
    nz = nb // 4
    z, y, c = b // 4, (b // 2) % 2, b % 2
    high = z // (nz // 2)
    edge = jnp.logical_or(z == 0, z == nz - 1)
    inner = jnp.logical_not(edge)
    zp = jnp.where(edge, z + 1 - 2 * high, z - 1 + 2 * high)
    zm = nz - 1 - z
    zq = nz - 1 - zp
    chunks, wide = buf.shape[0], buf.shape[5]
    experts = dbuf.shape[0]
    blocks = chunks // experts
    tokens = pooled.shape[0]
    half = tokens // 2
    piece = half // pieces
    tasks = tower_hidden.shape[0]
    deep_rows = w_second.shape[1]
    width = w_third.shape[2]
    splits = w_second.shape[2] // width

    def at(zz, yy, cc):
        return zz * 4 + yy * 2 + cc

    across, sib = at(z, 1 - y, c), at(z, y, 1 - c)

    def both(p, q):
        return jnp.logical_and(p, q)

    def either(p, q):
        return jnp.logical_or(p, q)

    def remote(src, dst, send, recv, tt, bb):
        return pltpu.make_async_remote_copy(
            src_ref=src, dst_ref=dst, send_sem=send, recv_sem=recv,
            device_id=(tt, bb), device_id_type=MESH,
        )

    def passed(n):
        count = 0
        for spot in SPOTS:
            count = count + jnp.where(n > spot, 1, 0)
        return count

    def zeroth(n):
        hit = n == SPOTS[0]
        for spot in SPOTS[1:]:
            hit = either(hit, n == spot)
        return hit

    def rank(n):
        return n - passed(n)

    def expert(n):
        return jnp.where(zeroth(n), 0, 1 + rank(n) // blocks)

    def block(n):
        return jnp.where(zeroth(n), passed(n), rank(n) % blocks)

    def own_copy(n):
        cols = pl.ds(pl.multiple_of(block(n) * wide, 128), wide)
        return pltpu.make_async_copy(
            w_first.at[expert(n), :, cols], buf.at[n, z, y, c], loc.at[n]
        )

    deep_copies = [
        pltpu.make_async_copy(
            w_second.at[:, :, pl.ds(h * width, width)],
            dbuf.at[:, z, y, c, pl.ds(h * deep_rows, deep_rows)], loc_deep.at[h],
        )
        for h in range(splits)
    ] + [
        pltpu.make_async_copy(
            w_third, dbuf.at[:, z, y, c, pl.ds(splits * deep_rows, w_third.shape[1])],
            loc_deep.at[splits],
        )
    ]
    tok_copy = pltpu.make_async_copy(pooled, tok.at[pl.ds(0, tokens)], loc_tok.at[0])

    for copy in deep_copies:
        copy.start()

    @pl.loop(0, chunks)
    def _(n):
        own_copy(n).start()

    tok_copy.start()

    barrier = pltpu.get_barrier_semaphore()
    for tt, bb in (
        (t, across), (t, sib), (t, at(zp, y, c)), (t, at(zm, y, c)), (1 - t, b),
        (1 - t, at(zp, y, c)),
    ):
        pl.semaphore_signal(barrier, inc=1, device_id=(tt, bb), device_id_type=MESH)
    pl.semaphore_wait(barrier, 6)

    swaps = [
        remote(gate, gate_rx, g_s.at[0], g_r.at[0], 1 - t, b),
        remote(tower_hidden, th_all.at[pl.ds(t * tasks, tasks)], g_s.at[1], g_r.at[1], 1 - t, b),
        remote(tower_out, to_all.at[t], g_s.at[2], g_r.at[2], 1 - t, b),
    ]
    for move in swaps:
        move.start()

    def chunk(n):
        return (lambda zz, yy: buf.at[n, zz, yy, c], lambda zz: buf.at[n, zz, :, c],
                n, zeroth(n), jnp.logical_not(zeroth(n)))

    def deep(e):
        return (lambda zz, yy: dbuf.at[e, zz, yy, c], lambda zz: dbuf.at[e, zz, :, c],
                chunks + e, e >= 0, e != 0)

    def hop(it, zz, yy, sem, bb):
        ref = it[0](zz, yy)
        return remote(ref, ref, sem, got.at[it[2], zz, yy], t, bb)

    def to_mid(it, zz, yy, key):
        return hop(it, zz, yy, z_s.at[it[2], key], at(zm, y, c))

    def to_pair(it, zz, yy, key):
        return hop(it, zz, yy, f_s.at[it[2], key], at(zp, y, c))

    def to_side(it, zz):
        return hop(it, zz, y, y_s.at[it[2], zz], across)

    def to_sib(it, zz):
        ref = it[1](zz)
        return remote(ref, ref, sib_s.at[it[2], zz], sib_r.at[it[2], zz], t, sib)

    def landed(it, zz, yy):
        to_pair(it, zz, yy, 0).wait_recv()

    def own(it):
        _, _, _, dup, ends = it
        to_side(it, z).start()

        @pl.when(inner)
        def _():
            to_mid(it, z, y, 0).start()

        @pl.when(either(edge, ends))
        def _():
            to_pair(it, z, y, 0).start()

    def finish(it):
        _, _, _, dup, ends = it
        landed(it, z, 1 - y)

        @pl.when(both(dup, inner))
        def _():
            to_mid(it, z, 1 - y, 1).start()

        @pl.when(both(dup, either(edge, ends)))
        def _():
            to_pair(it, z, 1 - y, 1).start()

        @pl.when(either(inner, ends))
        def _():
            to_sib(it, z).start()

    def feed(it):
        _, _, _, dup, ends = it
        landed(it, zp, y)
        to_mid(it, zp, y, 2).start()

        @pl.when(dup)
        def _():
            landed(it, zp, 1 - y)
            to_mid(it, zp, 1 - y, 3).start()
            to_sib(it, zp).start()

        @pl.when(jnp.logical_not(dup))
        def _():
            to_side(it, zp).start()

    def take(it, key, zz):
        _, _, _, dup, ends = it
        landed(it, zz, y)

        @pl.when(both(inner, ends))
        def _():
            to_pair(it, zz, y, key).start()

        @pl.when(dup)
        def _():
            landed(it, zz, 1 - y)

            @pl.when(both(inner, ends))
            def _():
                to_pair(it, zz, 1 - y, key + 1).start()

            to_sib(it, zz).start()

        @pl.when(jnp.logical_not(dup))
        def _():
            to_side(it, zz).start()

    def near(it):
        @pl.when(either(inner, it[4]))
        def _():
            take(it, 2, jnp.where(inner, zm, zp))

    def far(it):
        @pl.when(either(inner, it[4]))
        def _():
            take(it, 4, zq)

        @pl.when(both(edge, it[4]))
        def _():
            take(it, 2, zm)

    def cross(it):
        @pl.when(jnp.logical_not(it[3]))
        def _():
            for zz in (zp, zm, zq):
                landed(it, zz, 1 - y)
                to_sib(it, zz).start()

    def sib_wait(it):
        @pl.loop(0, nz)
        def _(zz):
            to_sib(it, zz).wait_recv()

    def stage(n, step):
        @pl.when(block(n) == 2)
        def _():
            step(deep(expert(n)))

        step(chunk(n))

    def own_at(n):
        own_copy(n).wait()
        stage(n, own)

    def tok_rows(h, p):
        return pl.ds(pl.multiple_of(h * half + p * piece, 16), piece)

    def far_rows(p):
        return pl.ds(pl.multiple_of(tokens + t * half + p * piece, 16), piece)

    def p_move(p):
        return remote(
            pooled.at[tok_rows(t, p)], tok.at[far_rows(p)], p_s.at[p], p_r.at[p], t, at(zp, y, c)
        )

    def q_move(p):
        rows = far_rows(p)
        return remote(tok.at[rows], tok.at[rows], q_s.at[p], q_r.at[p], 1 - t, b)

    for copy in deep_copies:
        copy.wait()
    own_ahead = jnp.where(edge, OWN_AHEAD_EDGE, OWN_AHEAD)

    @pl.loop(0, own_ahead)
    def _(n):
        own_at(n)

    @pl.when(edge)
    def _():
        @pl.loop(0, chunks)
        def _(n):
            @pl.when(n + OWN_AHEAD_EDGE < chunks)
            def _():
                own_at(n + OWN_AHEAD_EDGE)

            stage(n, finish)

            @pl.when(both(n > PIECE_LAG, n <= PIECE_LAG + pieces))
            def _():
                p_move(n - PIECE_LAG - 1).start()

    @pl.when(inner)
    def _():
        @pl.loop(0, PAIR_AHEAD)
        def _(n):
            stage(n, finish)

        @pl.loop(0, FEED_AHEAD)
        def _(n):
            stage(n, feed)

    tok_copy.wait()
    every = gate.shape[1]

    def o_move(e):
        slot = experts + e
        return remote(out_tx.at[e], out_rx.at[slot], o_s.at[e], o_r.at[slot], 1 - t, b)

    def narrow(e, hidden):
        w3 = dbuf[e, :, :, :, pl.ds(splits * deep_rows, w_third.shape[1]), :].reshape(-1, width)
        total = None
        for h in range(splits):
            w2 = dbuf[e, :, :, :, pl.ds(h * deep_rows, deep_rows), :].reshape(-1, width)
            second = jnp.maximum(dot(hidden, w2), 0.0).astype(BF16)
            part = dot(second, w3[h * width : (h + 1) * width])
            total = part if total is None else total + part
        return jnp.maximum(total, 0.0).astype(BF16)

    def widen(n, rows, kept):
        cols = pl.ds(pl.multiple_of(block(n) * wide, 128), wide)
        weights = buf[n].reshape(-1, wide)
        first[kept, cols] = jnp.maximum(dot(tok[rows, :], weights), 0.0).astype(BF16)

    def compute(n, g):
        owner = 1 - t if g == 0 else t
        base = jnp.where(zeroth(n), 0, 2 * tokens)
        rows = pl.ds(pl.multiple_of(owner * half, 16), half)
        kept = pl.ds(pl.multiple_of(base + owner * half, 16), half)
        widen(n, rows, kept)

        @pl.when(block(n) == blocks - 1)
        def _():
            e = expert(n)
            value = narrow(e, first[kept, :])
            if g == 0:
                out_tx[e] = value
                o_move(e).start()
            else:
                out_rx[e] = value

    part = half // 2

    def far_move(f, side):
        owner = t + (1 - side) * (1 - 2 * t)
        rows = pl.ds(pl.multiple_of(f * part, 16), part)
        return remote(
            out_tx.at[experts + side, rows], out_rx.at[(1 - side) * experts, rows],
            far_s.at[side, f], far_r.at[1 - side, f], owner, at(zp, y, c),
        )

    def compute_far(f, side):
        owner = t + (1 - side) * (1 - 2 * t)
        rows = pl.ds(pl.multiple_of(tokens + owner * half + f * part, 16), part)

        @pl.loop(0, blocks)
        def _(s):
            spot = SPOTS[0]
            for k in range(1, blocks):
                spot = jnp.where(s == k, SPOTS[k], spot)
            widen(spot, rows, rows)

        there = pl.ds(pl.multiple_of(f * part, 16), part)
        out_tx[experts + side, there, :] = narrow(0, first[rows, :])
        far_move(f, side).start()

    near_ahead = jnp.where(edge, NEAR_AHEAD_EDGE, NEAR_AHEAD)

    @pl.loop(0, near_ahead)
    def _(n):
        stage(n, near)

    cross_lag = jnp.where(edge, CROSS_LAG_EDGE, CROSS_LAG)
    work_lag = jnp.where(edge, WORK_LAG_EDGE, WORK_LAG)

    @pl.loop(0, chunks + max(WORK_LAG, WORK_LAG_EDGE))
    def _(i):
        @pl.when(inner)
        def _():
            @pl.when(i + OWN_AHEAD < chunks)
            def _():
                own_at(i + OWN_AHEAD)

            @pl.when(i + PAIR_AHEAD < chunks)
            def _():
                stage(i + PAIR_AHEAD, finish)

            @pl.when(i + FEED_AHEAD < chunks)
            def _():
                stage(i + FEED_AHEAD, feed)

        n = i - work_lag
        ready = both(both(n >= 0, n < chunks), either(inner, jnp.logical_not(zeroth(n))))

        @pl.when(ready)
        def _():
            stage(n, sib_wait)
            compute(n, 0)

        @pl.when(i + near_ahead < chunks)
        def _():
            stage(i + near_ahead, near)

        @pl.when(i == 1)
        def _():
            for swap in swaps:
                swap.wait_recv()
            th_all[pl.ds(t * tasks, tasks)] = tower_hidden[...]
            to_all[t] = tower_out[...]
            for e in range(experts):
                gate_all[e * every : (e + 1) * every, :] = gate[e].astype(F32)
                gate_all[(experts + e) * every : (experts + e + 1) * every, :] = gate_rx[e].astype(F32)
            mine = pl.ds(pl.multiple_of(t * half, 16), half)
            raw = jnp.exp(
                lax.dot_general(
                    tok[mine, :], gate_all[...].astype(BF16), (((1,), (1,)), ((), ())),
                    preferred_element_type=F32,
                )
            )
            lane = lax.broadcasted_iota(jnp.int32, raw.shape, 1)
            below = jnp.ones_like(raw)
            for j in range(every):
                own_task = lane % every == j
                total = jnp.sum(jnp.where(own_task, raw, 0.0), axis=1, keepdims=True)
                below = jnp.where(own_task, total, below)
            wts[...] = raw / below
            acc[...] = jnp.zeros_like(acc)

        @pl.when(i < chunks)
        def _():
            stage(i, far)

        @pl.when(ready)
        def _():
            compute(n, 1)

        k = i - cross_lag

        @pl.when(both(k >= 0, k < chunks))
        def _():
            stage(k, cross)

        @pl.when(both(inner, both(i > PASS_LAG, i <= PASS_LAG + pieces)))
        def _():
            p_move(i - PASS_LAG - 1).wait_recv()
            q_move(i - PASS_LAG - 1).start()

        for f in range(2):
            @pl.when(both(inner, i == FAR_STEPS[f]))
            def _():
                @pl.loop(f * pieces // 2, (f + 1) * pieces // 2)
                def _(p):
                    q_move(p).wait_recv()

        first_far = both(i >= FAR_STEPS[0], i < FAR_STEPS[0] + 2)
        second_far = both(i >= FAR_STEPS[1], i < FAR_STEPS[1] + 2)

        @pl.when(both(inner, either(first_far, second_far)))
        def _():
            f = jnp.where(i >= FAR_STEPS[1], 1, 0)
            compute_far(f, i - jnp.where(f == 1, FAR_STEPS[1], FAR_STEPS[0]))

    def accumulate(far, e):
        value = out_rx[far * experts + e].astype(F32)
        for j in range(every):
            col = (far * experts + e) * every + j
            acc[j] = acc[j] + wts[:, col : col + 1] * value

    def waiting(e):
        o_move(e).wait_recv()

    def waiting_far(far):
        for f in range(2):
            far_move(f, 1 - far).wait_recv()

    for e in range(1, experts):
        accumulate(0, e)
    for e in range(1, experts - 1):
        waiting(e)
        accumulate(1, e)
    pl.when(edge)(lambda: waiting_far(0))
    accumulate(0, 0)
    pl.when(edge)(lambda: waiting_far(1))
    pl.when(inner)(lambda: waiting(0))
    accumulate(1, 0)
    for swap in swaps:
        swap.wait_send()

    @pl.when(edge)
    def _():
        @pl.loop(0, pieces)
        def _(p):
            p_move(p).wait_send()

    @pl.when(inner)
    def _():
        @pl.loop(0, pieces)
        def _(p):
            q_move(p).wait_send()

        o_move(0).wait_send()
        for f in range(2):
            for side in range(2):
                far_move(f, side).wait_send()

    @pl.loop(1, experts)
    def _(e):
        o_move(e).wait_send()

    def sent(it):
        _, _, _, dup, ends = it
        to_side(it, z).wait_send()

        @pl.when(inner)
        def _():
            to_mid(it, z, y, 0).wait_send()
            to_mid(it, zp, y, 2).wait_send()

            @pl.when(dup)
            def _():
                to_mid(it, z, 1 - y, 1).wait_send()
                to_mid(it, zp, 1 - y, 3).wait_send()

            @pl.when(ends)
            def _():
                to_pair(it, zm, y, 2).wait_send()
                to_pair(it, zq, y, 4).wait_send()

                @pl.when(dup)
                def _():
                    to_pair(it, zm, 1 - y, 3).wait_send()
                    to_pair(it, zq, 1 - y, 5).wait_send()

        @pl.when(either(edge, ends))
        def _():
            to_pair(it, z, y, 0).wait_send()

            @pl.when(dup)
            def _():
                to_pair(it, z, 1 - y, 1).wait_send()

        @pl.when(jnp.logical_not(dup))
        def _():
            for zz in (zp, zm, zq):
                to_side(it, zz).wait_send()

        @pl.when(either(inner, ends))
        def _():
            @pl.loop(0, nz)
            def _(zz):
                to_sib(it, zz).wait_send()

    @pl.loop(0, chunks)
    def _(n):
        sent(chunk(n))

    @pl.loop(0, experts)
    def _(e):
        sent(deep(e))

    waiting(experts - 1)
    accumulate(1, experts - 1)

    for j in range(every):
        mix = acc[j].astype(BF16)
        tower = jnp.maximum(dot(mix, th_all[j]), 0.0).astype(BF16)
        vector = jnp.broadcast_to(to_all[j // tasks, j % tasks : j % tasks + 1, :], (16, tower.shape[1]))
        line = lax.dot_general(
            vector, tower, (((1,), (1,)), ((), ())), preferred_element_type=F32
        )
        res[j // tasks, j % tasks : j % tasks + 1, :] = line[:1]
    r_move = remote(res.at[1 - t], res_rx, r_s.at[0], r_r.at[0], 1 - t, b)
    r_move.start()
    out[:, pl.ds(pl.multiple_of(t * half, 128), half)] = res[t, 0:tasks, :]

    r_move.wait()
    out[:, pl.ds(pl.multiple_of((1 - t) * half, 128), half)] = res_rx[0:tasks, :]


def fused(nb, pooled, gate_weight, w_first, w_second, w_third, tower_hidden, tower_out):
    tokens, width_in = pooled.shape
    experts, rows, h1 = w_first.shape
    tasks = tower_hidden.shape[0]
    all_tasks = gate_weight.shape[2]
    deep_rows, deep_width = w_second.shape[1:]
    last_rows, last_width = w_third.shape[1:]
    nz = nb // 4
    wide = h1 // BLOCKS
    chunks = experts * BLOCKS
    items = chunks + experts
    half = tokens // 2
    splits = deep_width // last_width
    packed_rows = splits * deep_rows + last_rows
    dma = pltpu.SemaphoreType.DMA
    vmem = pl.BlockSpec(memory_space=pltpu.VMEM)
    anywhere = pl.BlockSpec(memory_space=pl.ANY)
    gate = jnp.transpose(gate_weight, (1, 2, 0))
    lines = pl.pallas_call(
        functools.partial(fused_kernel, nb, PIECES),
        out_shape=jax.ShapeDtypeStruct((tasks, tokens), F32),
        in_specs=[anywhere, vmem, anywhere, anywhere, anywhere, vmem, vmem],
        out_specs=vmem,
        scratch_shapes=[
            pltpu.VMEM((2 * tokens, width_in), BF16),
            pltpu.VMEM((chunks, nz, 2, 2, rows, wide), BF16),
            pltpu.VMEM((experts, nz, 2, 2, packed_rows, last_width), BF16),
            pltpu.VMEM((3 * tokens, h1), BF16),
            pltpu.VMEM((experts + 2, half, last_width), BF16),
            pltpu.VMEM((2 * experts, half, last_width), BF16),
            pltpu.VMEM(gate.shape, BF16),
            pltpu.VMEM((2 * experts * all_tasks, width_in), F32),
            pltpu.VMEM((half, 2 * experts * all_tasks), F32),
            pltpu.VMEM((all_tasks, half, last_width), F32),
            pltpu.VMEM((all_tasks,) + tower_hidden.shape[1:], BF16),
            pltpu.VMEM((2,) + tower_out.shape, BF16),
            pltpu.VMEM((2, 8, half), F32),
            pltpu.VMEM((8, half), F32),
            dma((chunks,)),
            dma((splits + 1,)),
            dma((1,)),
            dma((PIECES,)),
            dma((PIECES,)),
            dma((PIECES,)),
            dma((PIECES,)),
            dma((3,)),
            dma((3,)),
            dma((items, nz, 2)),
            dma((items, 4)),
            dma((items, nz)),
            dma((items, 6)),
            dma((items, nz)),
            dma((items, nz)),
            dma((experts,)),
            dma((2 * experts,)),
            dma((2, 2)),
            dma((2, 2)),
            dma((1,)),
            dma((1,)),
        ],
        compiler_params=pltpu.CompilerParams(
            collective_id=0, has_side_effects=True, vmem_limit_bytes=VMEM_BYTES
        ),
    )(pooled, gate, w_first, w_second, w_third, tower_hidden, tower_out)
    return lines.T


def gathered_first(pooled, gate_weight, w_first, w_second, w_third, tower_hidden, tower_out):
    tok_rows = pooled.shape[0]
    width_in = pooled.shape[1]
    local_experts = w_first.shape[0]
    all_tasks = gate_weight.shape[2]
    own_tasks = tower_hidden.shape[0]
    gathered = lax.all_gather(w_first, "batch", axis=1, tiled=True)
    deep_rows, deep_width = w_second.shape[1], w_second.shape[2]
    last_rows, last_width = w_third.shape[1], w_third.shape[2]
    halves = deep_width // last_width
    packed = jnp.concatenate(
        [w_second[:, :, i * last_width : (i + 1) * last_width] for i in range(halves)] + [w_third],
        axis=1,
    )
    gathered, packed = lax.optimization_barrier((gathered, packed))
    packed = lax.all_gather(packed, "batch", axis=1, tiled=False)
    second_all = jnp.concatenate(
        [packed[:, :, i * deep_rows : (i + 1) * deep_rows] for i in range(halves)], axis=3
    ).reshape(local_experts, -1, deep_width)
    third_all = packed[:, :, halves * deep_rows :].reshape(local_experts, -1, last_width)
    summed = jnp.einsum("tr,erh->eth", pooled, gathered, preferred_element_type=jnp.float32)
    first = jax.nn.relu(summed).astype(jnp.bfloat16)
    logits = jnp.dot(
        pooled,
        gate_weight.reshape(width_in, local_experts * all_tasks),
        preferred_element_type=jnp.float32,
    )
    weights = jnp.exp(logits.reshape(tok_rows, local_experts, all_tasks))
    gate_total = jnp.sum(weights, axis=1)
    columns = first
    second = jax.nn.relu(
        jnp.einsum(
            "etr,erh->eth",
            columns,
            second_all,
            preferred_element_type=jnp.float32,
        )
    ).astype(jnp.bfloat16)
    columns = second
    expert_out = jax.nn.relu(
        jnp.einsum(
            "etr,erh->eth",
            columns,
            third_all,
            preferred_element_type=jnp.float32,
        )
    ).astype(jnp.bfloat16)
    numer = jnp.einsum("tek,eth->tkh", weights, expert_out.astype(jnp.float32))
    groups = all_tasks // own_tasks
    me = lax.axis_index("task")
    numer_own = lax.dynamic_slice_in_dim(numer, me * own_tasks, own_tasks, 1)
    total_own = lax.dynamic_slice_in_dim(gate_total, me * own_tasks, own_tasks, 1)
    for shift in range(1, groups):
        ring = [(i, (i + shift) % groups) for i in range(groups)]
        other = lax.rem(me + shift, groups) * own_tasks
        numer_sent = lax.dynamic_slice_in_dim(numer, other, own_tasks, 1).astype(jnp.bfloat16)
        total_sent = lax.dynamic_slice_in_dim(gate_total, other, own_tasks, 1)
        numer_own = numer_own + lax.ppermute(numer_sent, "task", ring).astype(jnp.float32)
        total_own = total_own + lax.ppermute(total_sent, "task", ring)
    mix = (numer_own / total_own[:, :, None]).astype(jnp.bfloat16)
    tower = jax.nn.relu(
        jnp.einsum("tkh,khm->tkm", mix, tower_hidden, preferred_element_type=jnp.float32)
    ).astype(jnp.bfloat16)
    return jnp.einsum("tkm,km->tk", tower, tower_out, preferred_element_type=jnp.float32)


def fits(mesh, pooled, gate_weight, w_first, w_second, w_third):
    even = all(w.shape[1] % 16 == 0 for w in (w_first, w_second, w_third))
    tokens, experts = pooled.shape[0], w_first.shape[0]
    cut = tokens % (32 * PIECES) == 0 and tokens % 256 == 0 and experts >= 4
    lanes = w_first.shape[2] % (128 * BLOCKS) == 0 and w_second.shape[2] % w_third.shape[2] == 0
    wanted = (gate_weight.shape[1] * gate_weight.shape[2]) <= 64
    two = mesh.shape["task"] == 2 and gate_weight.shape[2] % 2 == 0
    held = (experts * (w_first.shape[1] * w_first.shape[2]) + tokens * pooled.shape[1] // 8) * 32
    return even and cut and lanes and wanted and two and mesh.shape["batch"] == 16 and held < 2**26


def solution(mesh):
    placed = (
        P("batch", None),
        P(None, "task", None),
        P("task", "batch", None),
        P("task", "batch", None),
        P("task", "batch", None),
        P("task", None, None),
        P("task", None),
    )

    def per_device(*args):
        if fits(mesh, *args[:5]):
            return fused(mesh.shape["batch"], *args)
        return gathered_first(*args)

    return jax.shard_map(
        per_device, mesh=mesh, in_specs=placed, out_specs=P("batch", "task"), check_vma=False
    )
```
